32 devices in a mesh: dom: 8 (over z, y), sub: 4 (over x, core).
Axes of the slice: x: 2, y: 2, z: 4, core: 2. Of those that a mesh axis runs over, the one named last changes fastest.
Arguments:
- node_state: bfloat16 [64, 32768], P(None, ('dom', 'sub')), may hold values from -6 to 6
- edge_state: bfloat16 [64, 98304], P(None, ('dom', 'sub')), may hold values from -6 to 6
- senders: int32 [98304], P(('dom', 'sub')), may hold values from 0 to 2559, as said below
- receivers: int32 [98304], P(('dom', 'sub')), may hold values from 0 to 1023
- send_index: int32 [32, 12, 128], P(('dom', 'sub')), may hold values from -1 to 1023, as said below
- node_cotangent: bfloat16 [64, 32768], P(None, ('dom', 'sub')), may hold values from -6 to 6
- edge_cotangent: bfloat16 [64, 98304], P(None, ('dom', 'sub')), may hold values from -6 to 6
- edge_first: bfloat16 [192, 64], replicated, may hold values from -0.4375 to 0.4375
- edge_bias: float32 [64], replicated, may hold values from -3 to 3
- edge_second: bfloat16 [64, 64], replicated, may hold values from -0.75 to 0.75
- edge_gain: float32 [64], replicated, may hold values from 0.1 to 1.9
- edge_shift: float32 [64], replicated, may hold values from -3 to 3
- node_first: bfloat16 [128, 64], replicated, may hold values from -0.5 to 0.5
- node_bias: float32 [64], replicated, may hold values from -3 to 3
- node_second: bfloat16 [64, 64], replicated, may hold values from -0.75 to 0.75
- node_gain: float32 [64], replicated, may hold values from 0.1 to 1.9
Outputs:
- delta_state: bfloat16 [64, 32768], P(None, ('dom', 'sub'))
- delta_edges: bfloat16 [64, 98304], P(None, ('dom', 'sub'))
- delta_edgefirst: float32 [192, 64], replicated
- delta_edgebias: float32 [64], replicated
- delta_edgesecond: float32 [64, 64], replicated
- delta_edgegain: float32 [64], replicated
- delta_edgeshift: float32 [64], replicated
- delta_nodefirst: float32 [128, 64], replicated
- delta_nodebias: float32 [64], replicated
- delta_nodesecond: float32 [64, 64], replicated
- delta_nodegain: float32 [64], replicated
- delta_nodeshift: float32 [64], replicated
The draws below stay inside these ranges and needn't reach their ends.
Inputs may be any that keep to these rules, and one draw needn't show every extreme that they name: `send_index`: block k = o * 4 + t of partition p = d * 4 + s lists own cells that p sends to the partition at dom index d + o - 1 and sub index t: live entries first, then -1. Blocks towards a dom index outside the mesh, and block 4 + s, hold only -1; every other block holds 32 to 128 live entries. Some partition receives a full block from every partition that sends to it. `senders`: an entry below 1024 is an own cell. An entry 1024 + k * 128 + j with k = o * 4 + u names ghost slot j of block k: the j-th entry of block o * 4 + s of the partition at dom index d + 1 - o and sub index u, and that entry is live.
All inputs are finite; a program needn't handle non-finite values.
Results may differ from the reference program's by a relative error of at most 0.0095.
Values may be sent and summed in bfloat16 or wider, within the bound.
A program may use at most 64 MiB of HBM per device.

```python
import math
import jax
import jax.numpy as jnp
from jax import lax

D = 64
HIDDEN_SIZE = 64
CELLS_DEV = 1024
HALO = 128
FACES_DEV = 3072
PARTITIONS = 32
PEERS = 12
GHOST = 1536
CELLS = 32768
FACES = 98304
N_DOM = 8
N_SUB = 4


def halo_counts(key):
    base_key = jax.random.fold_in(key, 7)
    count_key, target_key = jax.random.split(base_key)
    live_count = jax.random.randint(count_key, (PARTITIONS, PEERS), HALO // 4, HALO + 1)
    partition = jnp.arange(PARTITIONS, dtype=jnp.int32)[:, None]
    peer_slot = jnp.arange(PEERS, dtype=jnp.int32)[None, :]
    target_row = partition // N_SUB + peer_slot // N_SUB - 1
    sub_here = partition % N_SUB
    exists = (target_row >= 0) & (target_row < N_DOM) & jnp.logical_not((peer_slot // N_SUB == 1) & (peer_slot % N_SUB == sub_here))
    chosen = jax.random.randint(target_key, (), N_SUB, PARTITIONS)
    target = target_row * N_SUB + peer_slot % N_SUB
    receives_full = target == chosen
    counts = jnp.where(receives_full, HALO, live_count)
    return jnp.where(exists, counts, 0).astype(jnp.int32)


def draw_send_index(key, part):
    counts = halo_counts(key)
    cell_draw = jax.random.randint(jax.random.fold_in(key, 11), (PARTITIONS, PEERS, HALO), 0, CELLS_DEV)
    slot_position = jnp.arange(HALO, dtype=jnp.int32)[None, None, :]
    return jnp.where(slot_position < counts[:, :, None], cell_draw, -1).astype(jnp.int32)


def draw_senders(key, part):
    counts = halo_counts(key)
    partition = jnp.arange(PARTITIONS, dtype=jnp.int32)[:, None]
    peer_slot = jnp.arange(PEERS, dtype=jnp.int32)[None, :]
    source_row = partition // N_SUB + 1 - peer_slot // N_SUB
    source_ok = (source_row >= 0) & (source_row < N_DOM)
    source = jnp.clip(source_row * N_SUB + peer_slot % N_SUB, 0, PARTITIONS - 1)
    mirror_slot = peer_slot // N_SUB * N_SUB + partition % N_SUB
    incoming = jnp.where(source_ok, counts[source, mirror_slot], 0)
    key_list = jax.random.split(jax.random.fold_in(key, 23), 4)
    local_cells = jax.random.randint(key_list[0], (PARTITIONS, FACES_DEV), 0, CELLS_DEV)
    chosen_peer = jax.random.randint(key_list[1], (PARTITIONS, FACES_DEV), 0, PEERS)
    position = jax.random.randint(key_list[2], (PARTITIONS, FACES_DEV), 0, HALO)
    want_ghost = jax.random.randint(key_list[3], (PARTITIONS, FACES_DEV), 0, 8) == 0
    face_number = jnp.arange(FACES_DEV, dtype=jnp.int32)[None, :]
    last_face = face_number == FACES_DEV - 1
    chosen_peer = jnp.where(last_face, PEERS - 1, chosen_peer)
    available = jnp.take_along_axis(incoming, chosen_peer, axis=1)
    position = jnp.where(last_face, available - 1, position % jnp.maximum(available, 1))
    use_ghost = (want_ghost | last_face) & (available > 0)
    ghost_index = CELLS_DEV + chosen_peer * HALO + position
    return jnp.where(use_ghost, ghost_index, local_cells).reshape(-1).astype(jnp.int32)


def place_ends(values, own_key, low, largest):
    shape = values.shape
    spot = [jax.random.randint(jax.random.fold_in(own_key, axis), (), 0, shape[axis]) for axis in range(len(shape))]
    values = values.at[tuple(spot)].set(low)
    longest = shape.index(max(shape))
    spot[longest] = (spot[longest] + 1) % shape[longest]
    return values.at[tuple(spot)].set(largest)


def level_of(key, extent, cuts, low, largest):
    level, own = 1.0, jax.random.fold_in(key, 6)
    for axis_at, shards_of in cuts:
        heights = jnp.exp(jax.random.uniform(jax.random.fold_in(own, axis_at), (shards_of,), jnp.float32, low / len(cuts), largest / len(cuts)))
        level = level * jnp.repeat(heights, extent[axis_at] // shards_of).reshape([-1 if axis == axis_at else 1 for axis in range(len(extent))])
    return level


def scatter_about(rng, shape, deviation, most, cuts=(), kind=jnp.bfloat16):
    factor_of = level_of(rng, shape, cuts, -0.22, 0.18) if cuts else 1.0
    values = jax.random.normal(rng, shape, jnp.float32) * deviation * factor_of
    return jnp.minimum(jnp.maximum(values, -most), most).astype(kind)


def setup_inputs(seed: int = 0) -> dict:
    splits = jax.random.split(jax.random.key(seed), 17)
    return {
        "node_state": scatter_about(splits[0], (D, CELLS), 1.0, 6.0, ((1, 32),)),
        "edge_state": scatter_about(splits[1], (D, FACES), 1.0, 6.0, ((1, 32),)),
        "senders": draw_senders(jax.random.fold_in(splits[16], 71), 0),
        "receivers": place_ends(jax.random.randint(splits[3], (FACES,), 0, CELLS_DEV), jax.random.fold_in(splits[3], 1), 0, CELLS_DEV - 1).astype(jnp.int32),
        "send_index": draw_send_index(jax.random.fold_in(splits[16], 71), 0),
        "node_cotangent": scatter_about(splits[5], (D, CELLS), 1.0, 6.0, ((1, 32),)),
        "edge_cotangent": scatter_about(splits[6], (D, FACES), 1.0, 6.0, ((1, 32),)),
        "edge_first": scatter_about(splits[7], (3 * D, HIDDEN_SIZE), (3 * D) ** -0.5, 0.4375),
        "edge_bias": scatter_about(splits[8], (HIDDEN_SIZE,), 0.5, 3.0, (), jnp.float32),
        "edge_second": scatter_about(splits[9], (HIDDEN_SIZE, D), HIDDEN_SIZE ** -0.5, 0.75),
        "edge_gain": jnp.clip(1.0 + 0.18 * jax.random.normal(splits[10], (D,), jnp.float32), 0.1, 1.9),
        "edge_shift": scatter_about(splits[11], (D,), 0.5, 3.0, (), jnp.float32),
        "node_first": scatter_about(splits[12], (2 * D, HIDDEN_SIZE), (2 * D) ** -0.5, 0.5),
        "node_bias": scatter_about(splits[13], (HIDDEN_SIZE,), 0.5, 3.0, (), jnp.float32),
        "node_second": scatter_about(splits[14], (HIDDEN_SIZE, D), HIDDEN_SIZE ** -0.5, 0.75),
        "node_gain": jnp.clip(1.0 + 0.18 * jax.random.normal(splits[15], (D,), jnp.float32), 0.1, 1.9),
    }


EPSILON = 1e-05

def contract_first(first_operand, second_operand):
    return lax.dot_general(first_operand, second_operand, (((0,), (0,)), ((), ())), preferred_element_type=jnp.float32)

def contract_last(first_operand, second_operand):
    return lax.dot_general(first_operand, second_operand, (((1,), (1,)), ((), ())), preferred_element_type=jnp.float32)

def sigmoid_linear(values):
    return values * jax.nn.sigmoid(values)

def sigmoid_slope(values):
    logistic = jax.nn.sigmoid(values)
    return logistic * (1.0 + values * (1.0 - logistic))

def standardize(values):
    centered = values - lax.optimization_barrier(jnp.mean(values, axis=0, keepdims=True))
    spread = lax.rsqrt(lax.optimization_barrier(jnp.mean(centered * centered, axis=0, keepdims=True)) + EPSILON)
    return (centered * spread, spread)

def normalize_back(upstream, scaled, spread, gain_vector):
    gain_delta = lax.optimization_barrier(jnp.sum(upstream * scaled, axis=1))
    shift_delta = lax.optimization_barrier(jnp.sum(upstream, axis=1))
    weighted = upstream * gain_vector[:, None]
    result = spread * (weighted - lax.optimization_barrier(jnp.mean(weighted, axis=0, keepdims=True)) - scaled * lax.optimization_barrier(jnp.mean(weighted * scaled, axis=0, keepdims=True)))
    return (result, gain_delta, shift_delta)

def local_backward(extended, node_state, edge_state, senders, receivers, node_cotangent, edge_cotangent, edge_first, edge_bias, edge_second, edge_gain, edge_shift, node_first, node_bias, node_second, node_gain):
    features, cell_count = node_state.shape
    sender_rows = jnp.take(extended, senders, axis=1)
    receiver_rows = jnp.take(node_state, receivers, axis=1)
    stacked = jnp.concatenate([sender_rows, receiver_rows, edge_state], axis=0)
    edge_linear = contract_first(edge_first, stacked) + edge_bias[:, None]
    edge_active = sigmoid_linear(edge_linear).astype(jnp.bfloat16)
    edge_output = contract_first(edge_second, edge_active)
    edge_scaled, edge_spread = standardize(edge_output)
    message = (edge_scaled * edge_gain[:, None] + edge_shift[:, None]).astype(jnp.bfloat16)
    summed = jnp.zeros((features, cell_count), jnp.float32).at[:, receivers].add(message.astype(jnp.float32))
    node_input = jnp.concatenate([node_state, summed.astype(jnp.bfloat16)], axis=0)
    node_linear = contract_first(node_first, node_input) + node_bias[:, None]
    node_active = sigmoid_linear(node_linear).astype(jnp.bfloat16)
    node_output = contract_first(node_second, node_active)
    node_scaled, node_spread = standardize(node_output)
    upstream = node_cotangent.astype(jnp.float32)
    node_delta, nodegain_delta, nodeshift_delta = normalize_back(upstream, node_scaled, node_spread, node_gain)
    node_delta = node_delta.astype(jnp.bfloat16)
    nodesecond_delta = contract_last(node_active, node_delta)
    node_hidden = jnp.dot(node_second, node_delta, preferred_element_type=jnp.float32) * sigmoid_slope(node_linear)
    nodebias_delta = lax.optimization_barrier(jnp.sum(node_hidden, axis=1))
    node_hidden = node_hidden.astype(jnp.bfloat16)
    nodefirst_delta = contract_last(node_input, node_hidden)
    node_back = jnp.dot(node_first, node_hidden, preferred_element_type=jnp.float32)
    message_delta = edge_cotangent.astype(jnp.float32) + jnp.take(node_back[features:], receivers, axis=1)
    edge_delta, edgegain_delta, edgeshift_delta = normalize_back(message_delta, edge_scaled, edge_spread, edge_gain)
    edge_delta = edge_delta.astype(jnp.bfloat16)
    edgesecond_delta = contract_last(edge_active, edge_delta)
    edge_hidden = jnp.dot(edge_second, edge_delta, preferred_element_type=jnp.float32) * sigmoid_slope(edge_linear)
    edgebias_delta = lax.optimization_barrier(jnp.sum(edge_hidden, axis=1))
    edge_hidden = edge_hidden.astype(jnp.bfloat16)
    edgefirst_delta = contract_last(stacked, edge_hidden)
    edge_back = jnp.dot(edge_first, edge_hidden, preferred_element_type=jnp.float32)
    edge_result = (edge_cotangent.astype(jnp.float32) + edge_back[2 * features:]).astype(jnp.bfloat16)
    scattered = jnp.zeros(extended.shape, jnp.float32).at[:, senders].add(edge_back[:features])
    local_delta = scattered[:, :cell_count].at[:, receivers].add(edge_back[features:2 * features]) + node_back[:features] + upstream
    ghost_delta = scattered[:, cell_count:]
    partials = (edgefirst_delta, edgebias_delta, edgesecond_delta, edgegain_delta, edgeshift_delta, nodefirst_delta, nodebias_delta, nodesecond_delta, nodegain_delta, nodeshift_delta)
    return (local_delta, ghost_delta, edge_result, partials)

def reference(node_state, edge_state, senders, receivers, send_index, node_cotangent, edge_cotangent, edge_first, edge_bias, edge_second, edge_gain, edge_shift, node_first, node_bias, node_second, node_gain):
    features = node_state.shape[0]
    partition = jnp.arange(PARTITIONS, dtype=jnp.int32)[:, None]
    peer_slot = jnp.arange(PEERS, dtype=jnp.int32)[None, :]
    slot_position = jnp.arange(HALO, dtype=jnp.int32)[None, None, :]
    mirror_slot = peer_slot // N_SUB * N_SUB + partition % N_SUB
    source_row = partition // N_SUB + 1 - peer_slot // N_SUB
    source_ok = (source_row >= 0) & (source_row < N_DOM)
    source = jnp.clip(source_row * N_SUB + peer_slot % N_SUB, 0, PARTITIONS - 1)
    incoming = send_index[source, mirror_slot]
    live_in = source_ok[:, :, None] & (incoming >= 0)
    global_in = source[:, :, None] * CELLS_DEV + jnp.maximum(incoming, 0)
    gathered = jnp.take(node_state, global_in.reshape(-1).astype(jnp.int32), axis=1)
    ghost_cells = jnp.where(live_in.reshape(1, -1), gathered, jnp.zeros_like(gathered))
    weight_shapes = (edge_first.shape, edge_bias.shape, edge_second.shape, edge_gain.shape, edge_gain.shape, node_first.shape, node_bias.shape, node_second.shape, node_gain.shape, node_gain.shape)
    initial = (jnp.zeros((features, CELLS), jnp.float32), jnp.zeros((features, PARTITIONS * GHOST), jnp.float32), jnp.zeros((features, FACES), jnp.bfloat16), tuple((jnp.zeros(shape, jnp.float32) for shape in weight_shapes)))

    def one_partition(loop_index, carried):
        local_all, ghost_all, edge_all, weight_all = carried
        cell_start = (loop_index * CELLS_DEV).astype(jnp.int32)
        face_start = (loop_index * FACES_DEV).astype(jnp.int32)
        ghost_start = (loop_index * GHOST).astype(jnp.int32)
        state_block = lax.dynamic_slice_in_dim(node_state, cell_start, CELLS_DEV, 1)
        ghost_block = lax.dynamic_slice_in_dim(ghost_cells, ghost_start, GHOST, 1)
        extended = jnp.concatenate([state_block, ghost_block], axis=1)
        outcome = local_backward(extended, state_block, lax.dynamic_slice_in_dim(edge_state, face_start, FACES_DEV, 1), lax.dynamic_slice_in_dim(senders, face_start, FACES_DEV, 0), lax.dynamic_slice_in_dim(receivers, face_start, FACES_DEV, 0), lax.dynamic_slice_in_dim(node_cotangent, cell_start, CELLS_DEV, 1), lax.dynamic_slice_in_dim(edge_cotangent, face_start, FACES_DEV, 1), edge_first, edge_bias, edge_second, edge_gain, edge_shift, node_first, node_bias, node_second, node_gain)
        local_delta, ghost_delta, edge_result, partials = outcome
        local_all = lax.dynamic_update_slice_in_dim(local_all, local_delta, cell_start, 1)
        ghost_all = lax.dynamic_update_slice_in_dim(ghost_all, ghost_delta, ghost_start, 1)
        edge_all = lax.dynamic_update_slice_in_dim(edge_all, edge_result, face_start, 1)
        weight_all = tuple((running + portion for running, portion in zip(weight_all, partials)))
        return (local_all, ghost_all, edge_all, weight_all)
    local_all, ghost_all, edge_all, weight_all = lax.fori_loop(0, PARTITIONS, one_partition, initial)
    target_row = partition // N_SUB + peer_slot // N_SUB - 1
    target_ok = (target_row >= 0) & (target_row < N_DOM)
    target = jnp.clip(target_row * N_SUB + peer_slot % N_SUB, 0, PARTITIONS - 1)
    live_out = target_ok[:, :, None] & (send_index >= 0)
    from_index = (target * PEERS + mirror_slot)[:, :, None] * HALO + slot_position
    coming_back = jnp.take(ghost_all, from_index.reshape(-1).astype(jnp.int32), axis=1)
    coming_back = jnp.where(live_out.reshape(1, -1), coming_back, jnp.zeros_like(coming_back))
    to_index = partition[:, :, None] * CELLS_DEV + jnp.maximum(send_index, 0)
    local_all = local_all.at[:, to_index.reshape(-1).astype(jnp.int32)].add(coming_back)
    factor = 1.0 / math.sqrt(FACES)
    edgefirst_sum, edgebias_sum, edgesecond_sum, edgegain_sum, edgeshift_sum, nodefirst_sum, nodebias_sum, nodesecond_sum, nodegain_sum, nodeshift_sum = weight_all
    return (local_all.astype(jnp.bfloat16), edge_all, edgefirst_sum * factor, edgebias_sum * factor, edgesecond_sum * factor, edgegain_sum * factor, edgeshift_sum * factor, nodefirst_sum * factor, nodebias_sum * factor, nodesecond_sum * factor, nodegain_sum * factor, nodeshift_sum * factor)
```

```python
import functools
import math

import jax
import jax.numpy as jnp
from jax import lax
from jax.experimental import pallas as pl
from jax.experimental.pallas import tpu as pltpu
from jax.sharding import PartitionSpec as P

EPSILON = 1e-05
MESH = pl.DeviceIdType.MESH
BF = jnp.bfloat16
F32 = jnp.float32
LOW = 256
PIECE = 8


def nn(a, b):
    return lax.dot_general(a, b, (((1,), (0,)), ((), ())), preferred_element_type=F32)


def nt(a, b):
    return lax.dot_general(a, b, (((1,), (1,)), ((), ())), preferred_element_type=F32)


def flip(a):
    return a.astype(F32).T


def standardize(values):
    centered = values - jnp.mean(values, axis=0, keepdims=True)
    spread = lax.rsqrt(jnp.mean(centered * centered, axis=0, keepdims=True) + EPSILON)
    return centered * spread, spread


def normalize_back(upstream, scaled, spread, gain):
    weighted = upstream * gain
    return spread * (
        weighted
        - jnp.mean(weighted, axis=0, keepdims=True)
        - scaled * jnp.mean(weighted * scaled, axis=0, keepdims=True)
    )


def lively_and_slope(linear):
    half = 0.5 * linear
    tilt = jnp.tanh(half)
    logistic = 0.5 + 0.5 * tilt
    lively = half + half * tilt
    return lively, logistic + lively * (1.0 - logistic)


def fold_lanes(values):
    total = values[:, :128]
    for begin in range(128, values.shape[1], 128):
        total = total + values[:, begin : begin + 128]
    return total


def stack_blocks(table):
    return jnp.concatenate([table[:, i : i + LOW] for i in range(0, table.shape[1], LOW)], axis=0)


def write_selector(selector, at, index):
    width = index.shape[1]
    low = jnp.bitwise_and(index, LOW - 1)
    offset = jnp.broadcast_to(low, (16, width)) - lax.broadcasted_iota(jnp.int32, (16, width), 0)
    offset = offset.astype(F32).astype(BF)
    one, zero = jnp.ones((16, width), BF), jnp.zeros((16, width), BF)
    for begin in range(0, LOW, 16):
        selector[begin : begin + 16, at] = jnp.where(offset == jnp.asarray(begin, BF), one, zero)


def choose(stacked, high, first, base):
    features = base.shape[0]
    high = jnp.broadcast_to(high, base.shape)
    for i in range(stacked.shape[0] // features):
        base = jnp.where(high == first + i, stacked[i * features : (i + 1) * features], base)
    return base


def spread_blocks(values, high, blocks):
    high = jnp.concatenate([high] * (values.shape[0] // 16), axis=0)
    zero = jnp.zeros(values.shape, values.dtype)
    return jnp.concatenate([jnp.where(high == jnp.asarray(i, BF), values, zero) for i in blocks], axis=0)


def high_part(index):
    return jnp.right_shift(index, 8)


def high_rows(index):
    return jnp.broadcast_to(high_part(index), (16, index.shape[1])).astype(F32).astype(BF)


def halo_peers(dom, sub):
    d, s = lax.axis_index("dom"), lax.axis_index("sub")
    for o in (0, 2, 1):
        for r in range(sub):
            if o == 1 and r == 0:
                continue
            t = lax.rem(s + r, sub)
            target = d + (o - 1)
            yield o, t, target, (target >= 0) & (target < dom)


def halo_copy(outgoing, incoming, send_sem, recv_sem, source, landing, target, t):
    return pltpu.make_async_remote_copy(
        src_ref=outgoing.at[source],
        dst_ref=incoming.at[landing],
        send_sem=send_sem.at[source],
        recv_sem=recv_sem.at[landing],
        device_id=(target, t),
        device_id_type=MESH,
    )


def guarded(o, there, action):
    if o == 1:
        action()
    else:
        pl.when(there)(action)


def start_exchange(dom, sub, s, outgoing, incoming, send_sem, recv_sem, forward):
    for o, t, target, there in halo_peers(dom, sub):
        block = o if forward else 2 - o

        def start(block=block, t=t, target=target):
            halo_copy(outgoing, incoming, send_sem, recv_sem, block * sub + t, block * sub + s, target, t).start()

        guarded(o, there, start)


def clear_absent(dom, sub, s, incoming, forward):
    d = lax.axis_index("dom")
    incoming[sub + s] = jnp.zeros(incoming.shape[1:], incoming.dtype)
    for o in (0, 2):
        origin = d + 1 - o if forward else d + o - 1

        @pl.when((origin < 0) | (origin >= dom))
        def _():
            for u in range(sub):
                incoming[o * sub + u] = jnp.zeros(incoming.shape[1:], incoming.dtype)


def finish_exchange(dom, sub, s, outgoing, incoming, send_sem, recv_sem, forward):
    for o, t, target, there in halo_peers(dom, sub):
        block = 2 - o if forward else o

        def finish(block=block, t=t, target=target):
            halo_copy(outgoing, incoming, send_sem, recv_sem, block * sub + t, block * sub + t, target, t).wait_recv()

        guarded(o, there, finish)


def settle_exchange(dom, sub, s, outgoing, incoming, send_sem, recv_sem, forward):
    for o, t, target, there in halo_peers(dom, sub):
        block = o if forward else 2 - o

        def finish(block=block, t=t, target=target):
            halo_copy(outgoing, incoming, send_sem, recv_sem, block * sub + t, block * sub + t, target, t).wait_send()

        guarded(o, there, finish)


def edge_owner(count, j):
    return count // 2 - 8 + j


def node_owner(count, j):
    return j + jnp.where(j < 8, 0, count - 16) if not isinstance(j, int) else (j if j < 8 else count - 16 + j)


class Reduction:
    def __init__(self, count, sub, me, number, owner, owned, packed, landing, reduced, result, sems):
        self.count, self.sub, self.me = count, sub, me
        self.number, self.owner, self.owned = number, owner, owned
        self.packed, self.landing, self.reduced, self.result = packed, landing, reduced, result
        self.part_send, self.part_recv, self.whole_send, self.whole_recv = sems
        self.is_owner, self.mine = owned

    def device(self, rank):
        return (rank // self.sub, lax.rem(rank, self.sub))

    def part(self, j, source, rank):
        return pltpu.make_async_remote_copy(
            src_ref=self.packed.at[j],
            dst_ref=self.landing.at[source],
            send_sem=self.part_send.at[j],
            recv_sem=self.part_recv.at[source],
            device_id=self.device(rank),
            device_id_type=MESH,
        )

    def whole(self, j, rank):
        return pltpu.make_async_remote_copy(
            src_ref=self.reduced,
            dst_ref=self.result.at[j],
            send_sem=self.whole_send.at[rank],
            recv_sem=self.whole_recv.at[j],
            device_id=self.device(rank),
            device_id_type=MESH,
        )

    def send_parts(self):
        def body(j, carry):
            rank = self.owner(self.count, j)

            @pl.when(rank != self.me)
            def _():
                self.part(j, self.me, rank).start()

            return carry

        lax.fori_loop(0, self.number, body, 0)

    def others(self, action):
        def body(r, carry):
            rank = lax.rem(self.me + r, self.count)
            action(rank)
            return carry

        lax.fori_loop(1, self.count, body, 0)

    def reduce(self):
        @pl.when(self.is_owner)
        def _():
            def take(r, total):
                rank = lax.rem(self.me + r, self.count)
                self.part(self.mine, rank, rank).wait_recv()
                return total + self.landing[rank].astype(F32)

            total = lax.fori_loop(1, self.count, take, self.packed[self.mine].astype(F32))
            self.reduced[...] = total.astype(BF)
            self.result[self.mine] = total.astype(BF)
            self.others(lambda rank: self.whole(self.mine, rank).start())

    def settle(self):
        def body(j, carry):
            rank = self.owner(self.count, j)

            @pl.when(rank != self.me)
            def _():
                self.part(j, rank, rank).wait_send()
                self.whole(j, rank).wait_recv()

            return carry

        lax.fori_loop(0, self.number, body, 0)

        @pl.when(self.is_owner)
        def _():
            self.others(lambda rank: self.whole(self.mine, rank).wait_send())


def layer_kernel(
    dom, sub, chunk,
    node_in, edge_in, senders_in, receivers_in, index_in, node_cot_in, edge_cot_in,
    edge_first_in, edge_second_in, node_first_in, node_second_in,
    edge_bias_in, edge_gain_in, edge_shift_in, node_bias_in, node_gain_in,
    state_ref, edge_out_ref, edge_sum, node_sum,
    node_ref, edge_ref, senders_ref, receivers_ref, index_ref, node_cot_ref, edge_cot_ref,
    edge_first_ref, edge_second_ref, node_first_ref, node_second_ref,
    edge_bias_ref, edge_gain_ref, edge_shift_ref, node_bias_ref, node_gain_ref,
    outgoing, incoming, returning, returned,
    export_sel, sender_sel, receiver_sel, sender_high, receiver_high, export_high,
    stacked, slope, active, scaled_all, spread_all, summed, by_sender, by_receiver, grads, lanes, local,
    edge_packed, node_packed, edge_landing, node_landing, edge_reduced, node_reduced,
    load_sem, send_sem, recv_sem, back_send, back_recv,
    edge_part_send, edge_part_recv, edge_whole_send, edge_whole_recv,
    node_part_send, node_part_recv, node_whole_send, node_whole_recv,
):
    features, cells = node_ref.shape
    faces = edge_ref.shape[1]
    peers, _, halo = outgoing.shape
    ghosts = peers * halo
    own_blocks = cells // LOW
    ghost_blocks = ghosts // LOW
    per = LOW // halo
    chunks = faces // chunk
    d, s = lax.axis_index("dom"), lax.axis_index("sub")
    count = dom * sub
    me = d * sub + s
    barrier = pltpu.get_barrier_semaphore()

    sources = [node_in, index_in, senders_in, receivers_in, edge_in, edge_first_in, edge_second_in,
               edge_bias_in, edge_gain_in, edge_shift_in, node_cot_in, node_first_in, node_second_in,
               node_bias_in, node_gain_in, edge_cot_in]
    targets = [node_ref, index_ref, senders_ref, receivers_ref, edge_ref, edge_first_ref, edge_second_ref,
               edge_bias_ref, edge_gain_ref, edge_shift_ref, node_cot_ref, node_first_ref, node_second_ref,
               node_bias_ref, node_gain_ref, edge_cot_ref]
    loads = [pltpu.make_async_copy(a, b, load_sem.at[i]) for i, (a, b) in enumerate(zip(sources, targets))]
    for load in loads:
        load.start()

    def greet(r, carry):
        other = lax.rem(me + r, count)
        pl.semaphore_signal(
            barrier, inc=1, device_id=(other // sub, lax.rem(other, sub)), device_id_type=MESH
        )
        return carry

    lax.fori_loop(1, count, greet, 0)
    clear_absent(dom, sub, s, incoming, True)
    clear_absent(dom, sub, s, returned, False)
    loads[0].wait()
    loads[1].wait()

    def halves(i):
        return pl.ds(pl.multiple_of(i * LOW, LOW), LOW)

    table = stack_blocks(node_ref[...])

    def pick(i, carry):
        here = halves(i)
        index = index_ref[:, here]
        write_selector(export_sel, here, index)
        export_high[:, here] = high_rows(index)
        picked = choose(nn(table, export_sel[:, here]), high_part(index), 0, jnp.zeros((features, LOW), F32))
        picked = picked.astype(BF)
        for p in range(per):
            outgoing[i * per + p] = picked[:, p * halo : (p + 1) * halo]
        return carry

    for i in range(ghost_blocks):
        pick(i, 0)
    pl.semaphore_wait(barrier, count - 1)
    start_exchange(dom, sub, s, outgoing, incoming, send_sem, recv_sem, forward=True)

    for load in loads[2:]:
        load.wait()
    edge_first_t = edge_first_ref[...]
    edge_first = flip(edge_first_t).astype(BF)
    edge_second = edge_second_ref[...]
    edge_second_t = flip(edge_second).astype(BF)
    vectors = [edge_bias_ref, edge_gain_ref, edge_shift_ref, node_bias_ref, node_gain_ref]
    columns = jnp.concatenate([v[...] for v in vectors] + [jnp.zeros((3, features), F32)], axis=0).T
    edge_bias, edge_gain, edge_shift, node_bias, node_gain = (columns[:, i : i + 1] for i in range(5))

    def span(c):
        return pl.ds(pl.multiple_of(c * chunk, chunk), chunk)

    def prepare(c, carry):
        here = span(c)
        sender = senders_ref[:, here]
        receiver = receivers_ref[:, here]
        write_selector(sender_sel, here, sender)
        write_selector(receiver_sel, here, receiver)
        sender_high[:, here] = high_rows(sender)
        receiver_high[:, here] = high_rows(receiver)
        zero = jnp.zeros((features, chunk), F32)
        received = choose(nn(table, receiver_sel[:, here]), high_part(receiver), 0, zero).astype(BF)
        sent = choose(nn(table, sender_sel[:, here]), high_part(sender), 0, zero).astype(BF)
        stacked[:features, here] = sent
        stacked[features:, here] = received
        slope[:, here] = nn(edge_first_t[:, features:], jnp.concatenate([received, edge_ref[:, here]], axis=0)) + edge_bias
        return carry

    lax.fori_loop(0, chunks, prepare, 0)
    summed[...] = jnp.zeros(summed.shape, F32)
    finish_exchange(dom, sub, s, outgoing, incoming, send_sem, recv_sem, forward=True)
    ghost_table = jnp.concatenate(
        [jnp.concatenate([incoming[i * per + p] for p in range(per)], axis=1) for i in range(ghost_blocks)], axis=0
    )

    def forward(c, carry):
        here = span(c)
        sent = choose(
            nn(ghost_table, sender_sel[:, here]), high_part(senders_ref[:, here]), own_blocks,
            stacked[:features, here].astype(F32),
        ).astype(BF)
        stacked[:features, here] = sent
        lively, steep = lively_and_slope(nn(edge_first_t[:, :features], sent) + slope[:, here])
        lively = lively.astype(BF)
        slope[:, here] = steep
        active[:, here] = lively
        scaled, spread = standardize(nn(edge_second_t, lively))
        scaled_all[:, here] = scaled
        spread_all[:, here] = spread
        message = (scaled * edge_gain + edge_shift).astype(BF)
        message = spread_blocks(message, receiver_high[:, here], range(own_blocks))
        summed[...] += nt(message, receiver_sel[:, here])
        return carry

    lax.fori_loop(0, chunks, forward, 0)

    def unstack(values):
        return jnp.concatenate([values[i : i + features] for i in range(0, values.shape[0], features)], axis=1)

    node_first_t = node_first_ref[...]
    node_first = flip(node_first_t).astype(BF)
    node_second_t = flip(node_second_ref[...]).astype(BF)
    node_input = jnp.concatenate([node_ref[...], unstack(summed[...]).astype(BF)], axis=0)
    node_lively, node_slope = lively_and_slope(nn(node_first_t, node_input) + node_bias)
    node_active = node_lively.astype(BF)
    node_scaled, node_spread = standardize(nn(node_second_t, node_active))
    upstream = node_cot_ref[...].astype(F32)
    node_delta = normalize_back(upstream, node_scaled, node_spread, node_gain).astype(BF)
    node_hidden = nn(node_second_ref[...], node_delta) * node_slope
    lanes[3] = fold_lanes(upstream * node_scaled)
    lanes[4] = fold_lanes(upstream)
    lanes[5] = fold_lanes(node_hidden)
    node_hidden = node_hidden.astype(BF)
    node_back = nn(node_first, node_hidden)
    local[...] = node_back[:features] + upstream
    toward = node_back[features:]
    high = toward.astype(BF)
    low = (toward - high.astype(F32)).astype(BF)
    toward_high, toward_low = stack_blocks(high), stack_blocks(low)

    def columns_of(first):
        column = lax.broadcasted_iota(jnp.int32, (features, 128), 1)
        result = jnp.zeros((features, 128), F32)
        for i in range(3):
            result = jnp.where(column == i, jnp.sum(lanes[first + i], axis=1, keepdims=True), result)
        return result

    def pack(packed, begin, values):
        for j in range(values.shape[0] // PIECE):
            packed[begin + j] = values[j * PIECE : (j + 1) * PIECE].astype(BF)

    edge_number, node_number = edge_packed.shape[0], node_packed.shape[0]
    edge_mine = me - edge_owner(count, 0)
    node_mine = jnp.where(me < 8, me, me - (count - 16))
    edge_reduction = Reduction(
        count, sub, me, edge_number, edge_owner,
        ((edge_mine >= 0) & (edge_mine < edge_number), jnp.clip(edge_mine, 0, edge_number - 1)),
        edge_packed, edge_landing, edge_reduced, edge_sum,
        (edge_part_send, edge_part_recv, edge_whole_send, edge_whole_recv),
    )
    node_reduction = Reduction(
        count, sub, me, node_number, node_owner,
        ((me < 8) | (me >= count - 8), jnp.clip(node_mine, 0, node_number - 1)),
        node_packed, node_landing, node_reduced, node_sum,
        (node_part_send, node_part_recv, node_whole_send, node_whole_recv),
    )
    pack(node_packed, 0, nt(node_hidden, node_input))
    node_right = jnp.concatenate([nt(node_active, node_delta), columns_of(3)[:, :features]], axis=1)
    pack(node_packed, features // PIECE, node_right)
    node_reduction.send_parts()

    grads[...] = jnp.zeros(grads.shape, F32)
    for i in range(3):
        lanes[i] = jnp.zeros(lanes.shape[1:], F32)

    def backward(c, carry):
        here = span(c)
        zero = jnp.zeros((features, chunk), F32)
        gathered = nn(toward_high, receiver_sel[:, here]) + nn(toward_low, receiver_sel[:, here])
        delta = edge_cot_ref[:, here].astype(F32) + choose(gathered, high_part(receivers_ref[:, here]), 0, zero)
        scaled = scaled_all[:, here]
        lanes[0] += fold_lanes(delta * scaled)
        lanes[1] += fold_lanes(delta)
        edge_delta = normalize_back(delta, scaled, spread_all[:, here], edge_gain).astype(BF)
        grads[:, 192:] += nt(active[:, here], edge_delta)
        hidden = nn(edge_second, edge_delta) * slope[:, here]
        lanes[2] += fold_lanes(hidden)
        hidden = hidden.astype(BF)
        active[:, here] = hidden
        grads[:, :128] += nt(hidden, stacked[:, here])
        grads[:, 128:192] += nt(hidden, edge_ref[:, here])
        return carry

    lax.fori_loop(0, chunks, backward, 0)
    pack(edge_packed, 0, grads[:, :128])
    pack(edge_packed, features // PIECE, grads[:, 128:])
    edge_packed[edge_number - 1] = jnp.concatenate(
        [columns_of(0).T[:PIECE], jnp.zeros((PIECE, features), F32)], axis=1
    ).astype(BF)
    edge_reduction.send_parts()

    by_sender[...] = jnp.zeros(by_sender.shape, F32)
    by_receiver[...] = jnp.zeros(by_receiver.shape, F32)
    ghost_rows = ghost_blocks * features

    def scatter_ghosts(c, carry):
        here = span(c)
        values = spread_blocks(active[:, here], sender_high[:, here], range(own_blocks, own_blocks + ghost_blocks))
        by_sender[:ghost_rows] += nt(values, sender_sel[:, here])
        return carry

    lax.fori_loop(0, chunks, scatter_ghosts, 0)
    for i in range(ghost_blocks):
        back = nn(edge_first[:features], by_sender[i * features : (i + 1) * features].astype(BF)).astype(BF)
        for p in range(per):
            returning[i * per + p] = back[:, p * halo : (p + 1) * halo]
    start_exchange(dom, sub, s, returning, returned, back_send, back_recv, forward=False)

    def scatter_own(c, carry):
        here = span(c)
        hidden = active[:, here]
        by_sender[ghost_rows:] += nt(spread_blocks(hidden, sender_high[:, here], range(own_blocks)), sender_sel[:, here])
        by_receiver[...] += nt(spread_blocks(hidden, receiver_high[:, here], range(own_blocks)), receiver_sel[:, here])
        ahead = nn(edge_first[2 * features :], hidden)
        edge_out_ref[:, here] = (edge_cot_ref[:, here].astype(F32) + ahead).astype(BF)
        return carry

    lax.fori_loop(0, chunks, scatter_own, 0)
    both = jnp.concatenate([unstack(by_sender[ghost_rows:]), unstack(by_receiver[...])], axis=0).astype(BF)
    weights = jnp.concatenate([edge_first[:features], edge_first[features : 2 * features]], axis=1)
    local[...] += nn(weights, both)

    node_reduction.reduce()
    finish_exchange(dom, sub, s, returning, returned, back_send, back_recv, forward=False)
    exported = jnp.concatenate([returned[k] for k in range(peers)], axis=1)
    exported = spread_blocks(exported, export_high[...], range(own_blocks))
    state_ref[...] = (local[...] + unstack(nt(exported, export_sel[...]))).astype(BF)
    edge_reduction.reduce()
    settle_exchange(dom, sub, s, outgoing, incoming, send_sem, recv_sem, forward=True)
    settle_exchange(dom, sub, s, returning, returned, back_send, back_recv, forward=False)
    node_reduction.settle()
    edge_reduction.settle()


def unpack_kernel(
    factor, state_in, edge_in, edge_sum, node_sum,
    state_ref, edge_ref, edge_first_ref, edge_second_ref, node_first_ref, node_second_ref,
    edge_gain_ref, edge_shift_ref, edge_bias_ref, node_gain_ref, node_shift_ref, node_bias_ref,
):
    features = state_in.shape[0]
    pieces = features // PIECE
    state_ref[...] = state_in[...]
    edge_ref[...] = edge_in[...]

    def block(ref, begin):
        return jnp.concatenate([ref[begin + j] for j in range(pieces)], axis=0).astype(F32) * factor

    right = block(edge_sum, pieces)
    edge_first_ref[:, : 2 * features] = block(edge_sum, 0)
    edge_first_ref[:, 2 * features :] = right[:, :features]
    edge_second_ref[...] = right[:, features:]
    edge_vectors = edge_sum[2 * pieces].astype(F32) * factor
    node_first_ref[...] = block(node_sum, 0)
    right = block(node_sum, pieces)
    node_second_ref[...] = right[:, :features]
    node_vectors = right.T[features : features + PIECE]
    for i, ref in enumerate((edge_gain_ref, edge_shift_ref, edge_bias_ref)):
        ref[...] = edge_vectors[i : i + 1, :features]
    for i, ref in enumerate((node_gain_ref, node_shift_ref, node_bias_ref)):
        ref[...] = node_vectors[i : i + 1]


def on_device(
    dom, sub,
    node_state, edge_state, senders, receivers, send_index, node_cotangent, edge_cotangent,
    edge_first, edge_bias, edge_second, edge_gain, edge_shift, node_first, node_bias, node_second, node_gain,
):
    features, cells = node_state.shape
    faces = edge_state.shape[1]
    halo = send_index.shape[2]
    peers = 3 * sub
    ghosts = peers * halo
    count = dom * sub
    chunk = math.gcd(faces, 512)
    edge_number = 4 * features // 16 + 1
    node_number = 4 * features // 16
    vmem = pl.BlockSpec(memory_space=pltpu.VMEM)
    hbm = pl.BlockSpec(memory_space=pltpu.HBM)
    shape = jax.ShapeDtypeStruct
    dma = pltpu.SemaphoreType.DMA

    def line(vector):
        return vector.reshape(1, -1)

    operands = (
        node_state, edge_state, line(senders), line(receivers), line(send_index),
        node_cotangent, edge_cotangent, edge_first.T, edge_second, node_first.T, node_second,
        line(edge_bias), line(edge_gain), line(edge_shift), line(node_bias), line(node_gain),
    )
    own_rows = cells // LOW * features
    ghost_rows = ghosts // LOW * features
    state, edge_result, edge_total, node_total = pl.pallas_call(
        functools.partial(layer_kernel, dom, sub, chunk),
        out_shape=(
            shape((features, cells), BF),
            shape((features, faces), BF),
            shape((edge_number, PIECE, 128), BF),
            shape((node_number, PIECE, 128), BF),
        ),
        in_specs=[hbm] * 16,
        out_specs=(vmem,) * 4,
        scratch_shapes=[pltpu.VMEM(x.shape, x.dtype) for x in operands]
        + [pltpu.VMEM((peers, features, halo), BF)] * 4
        + [
            pltpu.VMEM((LOW, ghosts), BF),
            pltpu.VMEM((LOW, faces), BF),
            pltpu.VMEM((LOW, faces), BF),
            pltpu.VMEM((16, faces), BF),
            pltpu.VMEM((16, faces), BF),
            pltpu.VMEM((16, ghosts), BF),
            pltpu.VMEM((2 * features, faces), BF),
            pltpu.VMEM((features, faces), F32),
            pltpu.VMEM((features, faces), BF),
            pltpu.VMEM((features, faces), F32),
            pltpu.VMEM((1, faces), F32),
            pltpu.VMEM((own_rows, LOW), F32),
            pltpu.VMEM((ghost_rows + own_rows, LOW), F32),
            pltpu.VMEM((own_rows, LOW), F32),
            pltpu.VMEM((features, 4 * features), F32),
            pltpu.VMEM((6, features, 128), F32),
            pltpu.VMEM((features, cells), F32),
            pltpu.VMEM((edge_number, PIECE, 128), BF),
            pltpu.VMEM((node_number, PIECE, 128), BF),
            pltpu.VMEM((count, PIECE, 128), BF),
            pltpu.VMEM((count, PIECE, 128), BF),
            pltpu.VMEM((PIECE, 128), BF),
            pltpu.VMEM((PIECE, 128), BF),
        ]
        + [dma((16,))]
        + [dma((peers,))] * 4
        + [dma((edge_number,)), dma((count,)), dma((count,)), dma((edge_number,))]
        + [dma((node_number,)), dma((count,)), dma((count,)), dma((node_number,))],
        compiler_params=pltpu.CompilerParams(
            collective_id=0, has_side_effects=True, vmem_limit_bytes=32 * 1024 * 1024
        ),
        name="layer",
    )(*(pltpu.with_memory_space_constraint(x, pltpu.HBM) for x in operands))
    vector = shape((1, features), F32)
    results = pl.pallas_call(
        functools.partial(unpack_kernel, 1.0 / math.sqrt(faces * count)),
        out_shape=(
            shape((features, cells), BF),
            shape((features, faces), BF),
            shape(edge_first.shape[::-1], F32),
            shape(edge_second.shape, F32),
            shape(node_first.shape[::-1], F32),
            shape(node_second.shape, F32),
        )
        + (vector,) * 6,
        in_specs=[vmem] * 4,
        out_specs=(vmem,) * 12,
        compiler_params=pltpu.CompilerParams(vmem_limit_bytes=16 * 1024 * 1024),
        name="unpack",
    )(state, edge_result, edge_total, node_total)
    state, edge_result, edge_first_sum, edge_second_sum, node_first_sum, node_second_sum, *vectors = results
    vectors = [v.reshape(-1) for v in vectors]
    return (
        state, edge_result, edge_first_sum.T, vectors[2], edge_second_sum, vectors[0], vectors[1],
        node_first_sum.T, vectors[5], node_second_sum, vectors[3], vectors[4],
    )


def solution(mesh):
    split = P(None, ("dom", "sub"))
    faces = P(("dom", "sub"))
    return jax.shard_map(
        functools.partial(on_device, mesh.shape["dom"], mesh.shape["sub"]),
        mesh=mesh,
        in_specs=(split, split, faces, faces, P(("dom", "sub"), None, None), split, split) + (P(),) * 9,
        out_specs=(split, split) + (P(),) * 10,
        check_vma=False,
    )
```

```python
import functools
import math

import jax
import jax.numpy as jnp
from jax import lax
from jax.experimental import pallas as pl
from jax.experimental.pallas import tpu as pltpu
from jax.sharding import PartitionSpec as P

EPSILON = 1e-05
MESH = pl.DeviceIdType.MESH
BF = jnp.bfloat16
F32 = jnp.float32
LOW = 256
PIECE = 8


def nn(a, b):
    return lax.dot_general(a, b, (((1,), (0,)), ((), ())), preferred_element_type=F32)


def nt(a, b):
    return lax.dot_general(a, b, (((1,), (1,)), ((), ())), preferred_element_type=F32)


def flip(a):
    return a.astype(F32).T


def standardize(values):
    centered = values - jnp.mean(values, axis=0, keepdims=True)
    spread = lax.rsqrt(jnp.mean(centered * centered, axis=0, keepdims=True) + EPSILON)
    return centered * spread, spread


def normalize_back(upstream, scaled, spread, gain):
    weighted = upstream * gain
    return spread * (
        weighted
        - jnp.mean(weighted, axis=0, keepdims=True)
        - scaled * jnp.mean(weighted * scaled, axis=0, keepdims=True)
    )


def lively_and_slope(linear):
    half = 0.5 * linear
    tilt = jnp.tanh(half)
    logistic = 0.5 + 0.5 * tilt
    lively = half + half * tilt
    return lively, logistic + lively * (1.0 - logistic)


def fold_lanes(values):
    total = values[:, :128]
    for begin in range(128, values.shape[1], 128):
        total = total + values[:, begin : begin + 128]
    return total


def stack_blocks(table):
    return jnp.concatenate([table[:, i : i + LOW] for i in range(0, table.shape[1], LOW)], axis=0)


def write_selector(selector, at, index):
    width = index.shape[1]
    low = jnp.bitwise_and(index, LOW - 1)
    offset = jnp.broadcast_to(low, (16, width)) - lax.broadcasted_iota(jnp.int32, (16, width), 0)
    offset = offset.astype(F32).astype(BF)
    one, zero = jnp.ones((16, width), BF), jnp.zeros((16, width), BF)
    for begin in range(0, LOW, 16):
        selector[begin : begin + 16, at] = jnp.where(offset == jnp.asarray(begin, BF), one, zero)


def choose(stacked, high, first, base):
    features = base.shape[0]
    high = jnp.broadcast_to(high, base.shape)
    for i in range(stacked.shape[0] // features):
        base = jnp.where(high == first + i, stacked[i * features : (i + 1) * features], base)
    return base


def spread_blocks(values, high, blocks):
    high = jnp.concatenate([high] * (values.shape[0] // 16), axis=0)
    zero = jnp.zeros(values.shape, values.dtype)
    return jnp.concatenate([jnp.where(high == jnp.asarray(i, BF), values, zero) for i in blocks], axis=0)


def high_part(index):
    return jnp.right_shift(index, 8)


def high_rows(index):
    return jnp.broadcast_to(high_part(index), (16, index.shape[1])).astype(F32).astype(BF)


def halo_peers(dom, sub):
    d, s = lax.axis_index("dom"), lax.axis_index("sub")
    for o in (0, 2, 1):
        for r in range(sub):
            if o == 1 and r == 0:
                continue
            t = lax.rem(s + r, sub)
            target = d + (o - 1)
            yield o, t, target, (target >= 0) & (target < dom)


def guarded(o, there, action):
    if o == 1:
        action()
    else:
        pl.when(there)(action)


def start_exchange(dom, sub, s, outgoing, incoming, send_sem, recv_sem, forward):
    for o, t, target, there in halo_peers(dom, sub):
        block = o if forward else 2 - o

        def start(block=block, t=t, target=target):
            pltpu.make_async_remote_copy(
                src_ref=outgoing.at[block * sub + t],
                dst_ref=incoming.at[block * sub + s],
                send_sem=send_sem.at[block],
                recv_sem=recv_sem.at[block],
                device_id=(target, t),
                device_id_type=MESH,
            ).start()

        guarded(o, there, start)


def clear_absent(dom, sub, s, incoming, forward):
    d = lax.axis_index("dom")
    incoming[sub + s] = jnp.zeros(incoming.shape[1:], incoming.dtype)
    for o in (0, 2):
        origin = d + 1 - o if forward else d + o - 1

        @pl.when((origin < 0) | (origin >= dom))
        def _():
            for u in range(sub):
                incoming[o * sub + u] = jnp.zeros(incoming.shape[1:], incoming.dtype)


def await_bytes(ref, sem):
    pltpu.make_async_copy(ref, ref, sem).wait()


def settle_exchange(dom, sub, blocks, sem, ahead):
    d = lax.axis_index("dom")
    for o in (1, 0, 2):
        row = d + o - 1 if ahead else d + 1 - o
        number = sub - 1 if o == 1 else sub

        def finish(o=o, number=number):
            await_bytes(blocks.at[pl.ds(o * sub, number)], sem.at[o])

        guarded(o, (row >= 0) & (row < dom), finish)


def edge_owner(count, j):
    return count // 2 - 8 + j


def node_owner(count, j):
    return jnp.where(j < 8, j, count - 16 + j)


class Reduction:
    def __init__(self, count, sub, me, owner, is_owner, mine, packed, landing, reduced, result, sems):
        self.count, self.sub, self.me = count, sub, me
        self.number = packed.shape[0]
        self.owner, self.is_owner, self.mine = owner, is_owner, jnp.clip(mine, 0, self.number - 1)
        self.packed, self.landing, self.reduced, self.result, self.sems = packed, landing, reduced, result, sems

    def device(self, rank):
        return (rank // self.sub, lax.rem(rank, self.sub))

    def send_parts(self):
        def body(j, carry):
            rank = self.owner(self.count, j)

            @pl.when(rank != self.me)
            def _():
                pltpu.make_async_remote_copy(
                    src_ref=self.packed.at[j],
                    dst_ref=self.landing.at[lax.rem(self.me - rank + self.count, self.count) - 1],
                    send_sem=self.sems.at[0],
                    recv_sem=self.sems.at[1],
                    device_id=self.device(rank),
                    device_id_type=MESH,
                ).start()

            return carry

        lax.fori_loop(0, self.number, body, 0)

    def reduce(self):
        @pl.when(self.is_owner)
        def _():
            await_bytes(self.landing, self.sems.at[1])
            total = self.packed[self.mine].astype(F32) + jnp.sum(self.landing[...].astype(F32), axis=0)
            self.reduced[...] = total.astype(BF)
            self.result[self.mine] = total.astype(BF)

            def body(k, carry):
                rank = lax.rem(self.me + 1 + lax.rem(k + self.count // 2, self.count - 1), self.count)
                pltpu.make_async_remote_copy(
                    src_ref=self.reduced,
                    dst_ref=self.result.at[self.mine],
                    send_sem=self.sems.at[2],
                    recv_sem=self.sems.at[3],
                    device_id=self.device(rank),
                    device_id_type=MESH,
                ).start()
                return carry

            lax.fori_loop(0, self.count - 1, body, 0)

    def settle(self):
        @pl.when(self.is_owner)
        def _():
            await_bytes(self.packed.at[pl.ds(0, self.number - 1)], self.sems.at[0])
            await_bytes(self.landing, self.sems.at[2])
            await_bytes(self.result.at[pl.ds(0, self.number - 1)], self.sems.at[3])

        @pl.when(jnp.logical_not(self.is_owner))
        def _():
            await_bytes(self.packed, self.sems.at[0])
            await_bytes(self.result, self.sems.at[3])


def layer_kernel(
    dom, sub, chunk,
    node_in, edge_in, senders_in, receivers_in, index_in, node_cot_in, edge_cot_in,
    edge_first_in, edge_second_in, node_first_in, node_second_in,
    edge_bias_in, edge_gain_in, edge_shift_in, node_bias_in, node_gain_in,
    state_ref, edge_out_ref, edge_sum, node_sum,
    node_ref, edge_ref, senders_ref, receivers_ref, index_ref, node_cot_ref, edge_cot_ref,
    edge_first_ref, edge_second_ref, node_first_ref, node_second_ref,
    edge_bias_ref, edge_gain_ref, edge_shift_ref, node_bias_ref, node_gain_ref,
    outgoing, incoming, returning, returned,
    export_sel, sender_sel, receiver_sel, sender_high, receiver_high, export_high,
    stacked, slope, active, scaled_all, spread_all, summed, by_sender, by_receiver, grads, lanes, local,
    edge_packed, node_packed, edge_landing, node_landing, edge_reduced, node_reduced,
    load_sem, send_sem, recv_sem, back_send, back_recv,
    edge_sems, node_sems,
):
    features, cells = node_ref.shape
    faces = edge_ref.shape[1]
    peers, _, halo = outgoing.shape
    ghosts = peers * halo
    own_blocks = cells // LOW
    ghost_blocks = ghosts // LOW
    per = LOW // halo
    chunks = faces // chunk
    d, s = lax.axis_index("dom"), lax.axis_index("sub")
    count = dom * sub
    me = d * sub + s
    barrier = pltpu.get_barrier_semaphore()

    sources = [node_in, index_in, senders_in, receivers_in, edge_in, edge_first_in, edge_second_in,
               edge_bias_in, edge_gain_in, edge_shift_in, node_cot_in, node_first_in, node_second_in,
               node_bias_in, node_gain_in, edge_cot_in]
    targets = [node_ref, index_ref, senders_ref, receivers_ref, edge_ref, edge_first_ref, edge_second_ref,
               edge_bias_ref, edge_gain_ref, edge_shift_ref, node_cot_ref, node_first_ref, node_second_ref,
               node_bias_ref, node_gain_ref, edge_cot_ref]
    loads = [pltpu.make_async_copy(a, b, load_sem.at[i]) for i, (a, b) in enumerate(zip(sources, targets))]
    for load in loads:
        load.start()

    def greet(r, carry):
        other = lax.rem(me + r, count)
        pl.semaphore_signal(
            barrier, inc=1, device_id=(other // sub, lax.rem(other, sub)), device_id_type=MESH
        )
        return carry

    lax.fori_loop(1, count, greet, 0)
    clear_absent(dom, sub, s, incoming, True)
    clear_absent(dom, sub, s, returned, False)
    loads[0].wait()
    loads[1].wait()

    def halves(i):
        return pl.ds(pl.multiple_of(i * LOW, LOW), LOW)

    table = stack_blocks(node_ref[...])

    def pick(i, carry):
        here = halves(i)
        index = index_ref[:, here]
        write_selector(export_sel, here, index)
        export_high[:, here] = high_rows(index)
        picked = choose(nn(table, export_sel[:, here]), high_part(index), 0, jnp.zeros((features, LOW), F32))
        picked = picked.astype(BF)
        for p in range(per):
            outgoing[i * per + p] = picked[:, p * halo : (p + 1) * halo]
        return carry

    for i in range(ghost_blocks):
        pick(i, 0)
    pl.semaphore_wait(barrier, count - 1)
    start_exchange(dom, sub, s, outgoing, incoming, send_sem, recv_sem, forward=True)

    for load in loads[2:]:
        load.wait()
    edge_first_t = edge_first_ref[...]
    edge_first = flip(edge_first_t).astype(BF)
    edge_second = edge_second_ref[...]
    edge_second_t = flip(edge_second).astype(BF)
    vectors = [edge_bias_ref, edge_gain_ref, edge_shift_ref, node_bias_ref, node_gain_ref]
    columns = jnp.concatenate([v[...] for v in vectors] + [jnp.zeros((3, features), F32)], axis=0).T
    edge_bias, edge_gain, edge_shift, node_bias, node_gain = (columns[:, i : i + 1] for i in range(5))

    def span(c):
        return pl.ds(pl.multiple_of(c * chunk, chunk), chunk)

    everything = pl.ds(0, faces)

    def prepare(here):
        sender = senders_ref[:, here]
        receiver = receivers_ref[:, here]
        write_selector(sender_sel, here, sender)
        write_selector(receiver_sel, here, receiver)
        sender_high[:, here] = high_rows(sender)
        receiver_high[:, here] = high_rows(receiver)
        zero = jnp.zeros((features, faces), F32)
        received = choose(nn(table, receiver_sel[:, here]), high_part(receiver), 0, zero).astype(BF)
        sent = choose(nn(table, sender_sel[:, here]), high_part(sender), 0, zero).astype(BF)
        stacked[:features, here] = sent
        stacked[features:, here] = received
        slope[:, here] = nn(edge_first_t[:, features:], jnp.concatenate([received, edge_ref[:, here]], axis=0)) + edge_bias

    prepare(everything)
    settle_exchange(dom, sub, incoming, recv_sem, False)
    ghost_table = jnp.concatenate(
        [jnp.concatenate([incoming[i * per + p] for p in range(per)], axis=1) for i in range(ghost_blocks)], axis=0
    )

    def forward(here):
        sent = choose(
            nn(ghost_table, sender_sel[:, here]), high_part(senders_ref[:, here]), own_blocks,
            stacked[:features, here].astype(F32),
        ).astype(BF)
        stacked[:features, here] = sent
        lively, steep = lively_and_slope(nn(edge_first_t[:, :features], sent) + slope[:, here])
        lively = lively.astype(BF)
        slope[:, here] = steep
        active[:, here] = lively
        scaled, spread = standardize(nn(edge_second_t, lively))
        scaled_all[:, here] = scaled
        spread_all[:, here] = spread
        message = (scaled * edge_gain + edge_shift).astype(BF)
        message = spread_blocks(message, receiver_high[:, here], range(own_blocks))
        summed[...] = nt(message, receiver_sel[:, here])

    forward(everything)

    def unstack(values):
        return jnp.concatenate([values[i : i + features] for i in range(0, values.shape[0], features)], axis=1)

    node_first_t = node_first_ref[...]
    node_first = flip(node_first_t).astype(BF)
    node_second_t = flip(node_second_ref[...]).astype(BF)
    node_input = jnp.concatenate([node_ref[...], unstack(summed[...]).astype(BF)], axis=0)
    node_lively, node_slope = lively_and_slope(nn(node_first_t, node_input) + node_bias)
    node_active = node_lively.astype(BF)
    node_scaled, node_spread = standardize(nn(node_second_t, node_active))
    upstream = node_cot_ref[...].astype(F32)
    node_delta = normalize_back(upstream, node_scaled, node_spread, node_gain).astype(BF)
    node_hidden = nn(node_second_ref[...], node_delta) * node_slope
    lanes[3] = fold_lanes(upstream * node_scaled)
    lanes[4] = fold_lanes(upstream)
    lanes[5] = fold_lanes(node_hidden)
    node_hidden = node_hidden.astype(BF)
    node_back = nn(node_first, node_hidden)
    local[...] = node_back[:features] + upstream
    toward = node_back[features:]
    high = toward.astype(BF)
    low = (toward - high.astype(F32)).astype(BF)
    toward_high, toward_low = stack_blocks(high), stack_blocks(low)

    def columns_of(first):
        column = lax.broadcasted_iota(jnp.int32, (features, 128), 1)
        result = jnp.zeros((features, 128), F32)
        for i in range(3):
            result = jnp.where(column == i, jnp.sum(lanes[first + i], axis=1, keepdims=True), result)
        return result

    def pack(packed, begin, values):
        for j in range(values.shape[0] // PIECE):
            packed[begin + j] = values[j * PIECE : (j + 1) * PIECE].astype(BF)

    edge_number = edge_packed.shape[0]
    edge_mine = me - edge_owner(count, 0)
    edge_reduction = Reduction(
        count, sub, me, edge_owner, (edge_mine >= 0) & (edge_mine < edge_number), edge_mine,
        edge_packed, edge_landing, edge_reduced, edge_sum, edge_sems,
    )
    node_reduction = Reduction(
        count, sub, me, node_owner, (me < 8) | (me >= count - 8), jnp.where(me < 8, me, me - (count - 16)),
        node_packed, node_landing, node_reduced, node_sum, node_sems,
    )
    pack(node_packed, 0, nt(node_hidden, node_input))
    node_right = jnp.concatenate([nt(node_active, node_delta), columns_of(3)[:, :features]], axis=1)
    pack(node_packed, features // PIECE, node_right)
    node_reduction.send_parts()


    def backward(here):
        zero = jnp.zeros((features, faces), F32)
        gathered = nn(toward_high, receiver_sel[:, here]) + nn(toward_low, receiver_sel[:, here])
        delta = edge_cot_ref[:, here].astype(F32) + choose(gathered, high_part(receivers_ref[:, here]), 0, zero)
        scaled = scaled_all[:, here]
        lanes[0] = fold_lanes(delta * scaled)
        lanes[1] = fold_lanes(delta)
        edge_delta = normalize_back(delta, scaled, spread_all[:, here], edge_gain).astype(BF)
        grads[:, 192:] = nt(active[:, here], edge_delta)
        hidden = nn(edge_second, edge_delta) * slope[:, here]
        lanes[2] = fold_lanes(hidden)
        hidden = hidden.astype(BF)
        active[:, here] = hidden
        grads[:, :128] = nt(hidden, stacked[:, here])
        grads[:, 128:192] = nt(hidden, edge_ref[:, here])

    backward(everything)
    pack(edge_packed, 0, grads[:, :128])
    pack(edge_packed, features // PIECE, grads[:, 128:])
    edge_packed[edge_number - 1] = jnp.concatenate(
        [columns_of(0).T[:PIECE], jnp.zeros((PIECE, features), F32)], axis=1
    ).astype(BF)
    edge_reduction.send_parts()

    by_sender[...] = jnp.zeros(by_sender.shape, F32)
    by_receiver[...] = jnp.zeros(by_receiver.shape, F32)
    ghost_rows = ghost_blocks * features

    def scatter_ghosts(c, carry):
        here = span(c)
        values = spread_blocks(active[:, here], sender_high[:, here], range(own_blocks, own_blocks + ghost_blocks))
        by_sender[:ghost_rows] += nt(values, sender_sel[:, here])
        return carry

    lax.fori_loop(0, chunks, scatter_ghosts, 0)
    for i in range(ghost_blocks):
        back = nn(edge_first[:features], by_sender[i * features : (i + 1) * features].astype(BF)).astype(BF)
        for p in range(per):
            returning[i * per + p] = back[:, p * halo : (p + 1) * halo]
    start_exchange(dom, sub, s, returning, returned, back_send, back_recv, forward=False)

    def scatter_own(c, carry):
        here = span(c)
        hidden = active[:, here]
        by_sender[ghost_rows:] += nt(spread_blocks(hidden, sender_high[:, here], range(own_blocks)), sender_sel[:, here])
        by_receiver[...] += nt(spread_blocks(hidden, receiver_high[:, here], range(own_blocks)), receiver_sel[:, here])
        ahead = nn(edge_first[2 * features :], hidden)
        edge_out_ref[:, here] = (edge_cot_ref[:, here].astype(F32) + ahead).astype(BF)
        return carry

    lax.fori_loop(0, chunks, scatter_own, 0)
    both = jnp.concatenate([unstack(by_sender[ghost_rows:]), unstack(by_receiver[...])], axis=0).astype(BF)
    weights = jnp.concatenate([edge_first[:features], edge_first[features : 2 * features]], axis=1)
    local[...] += nn(weights, both)

    node_reduction.reduce()
    edge_reduction.reduce()
    settle_exchange(dom, sub, returned, back_recv, True)
    exported = jnp.concatenate([returned[k] for k in range(peers)], axis=1)
    exported = spread_blocks(exported, export_high[...], range(own_blocks))
    state_ref[...] = (local[...] + unstack(nt(exported, export_sel[...]))).astype(BF)
    settle_exchange(dom, sub, outgoing, send_sem, True)
    settle_exchange(dom, sub, returning, back_send, False)
    node_reduction.settle()
    edge_reduction.settle()


def unpack_kernel(
    factor, state_in, edge_in, edge_sum, node_sum,
    state_ref, edge_ref, edge_first_ref, edge_second_ref, node_first_ref, node_second_ref,
    edge_gain_ref, edge_shift_ref, edge_bias_ref, node_gain_ref, node_shift_ref, node_bias_ref,
):
    features = state_in.shape[0]
    pieces = features // PIECE
    state_ref[...] = state_in[...]
    edge_ref[...] = edge_in[...]

    def block(ref, begin):
        return jnp.concatenate([ref[begin + j] for j in range(pieces)], axis=0).astype(F32) * factor

    right = block(edge_sum, pieces)
    edge_first_ref[:, : 2 * features] = block(edge_sum, 0)
    edge_first_ref[:, 2 * features :] = right[:, :features]
    edge_second_ref[...] = right[:, features:]
    edge_vectors = edge_sum[2 * pieces].astype(F32) * factor
    node_first_ref[...] = block(node_sum, 0)
    right = block(node_sum, pieces)
    node_second_ref[...] = right[:, :features]
    node_vectors = right.T[features : features + PIECE]
    for i, ref in enumerate((edge_gain_ref, edge_shift_ref, edge_bias_ref)):
        ref[...] = edge_vectors[i : i + 1, :features]
    for i, ref in enumerate((node_gain_ref, node_shift_ref, node_bias_ref)):
        ref[...] = node_vectors[i : i + 1]


def on_device(
    dom, sub,
    node_state, edge_state, senders, receivers, send_index, node_cotangent, edge_cotangent,
    edge_first, edge_bias, edge_second, edge_gain, edge_shift, node_first, node_bias, node_second, node_gain,
):
    features, cells = node_state.shape
    faces = edge_state.shape[1]
    halo = send_index.shape[2]
    peers = 3 * sub
    ghosts = peers * halo
    count = dom * sub
    chunk = math.gcd(faces, 1536)
    edge_number = 4 * features // 16 + 1
    node_number = 4 * features // 16
    vmem = pl.BlockSpec(memory_space=pltpu.VMEM)
    hbm = pl.BlockSpec(memory_space=pltpu.HBM)
    shape = jax.ShapeDtypeStruct
    dma = pltpu.SemaphoreType.DMA

    def line(vector):
        return vector.reshape(1, -1)

    operands = (
        node_state, edge_state, line(senders), line(receivers), line(send_index),
        node_cotangent, edge_cotangent, edge_first.T, edge_second, node_first.T, node_second,
        line(edge_bias), line(edge_gain), line(edge_shift), line(node_bias), line(node_gain),
    )
    own_rows = cells // LOW * features
    ghost_rows = ghosts // LOW * features
    state, edge_result, edge_total, node_total = pl.pallas_call(
        functools.partial(layer_kernel, dom, sub, chunk),
        out_shape=(
            shape((features, cells), BF),
            shape((features, faces), BF),
            shape((edge_number, PIECE, 128), BF),
            shape((node_number, PIECE, 128), BF),
        ),
        in_specs=[hbm] * 16,
        out_specs=(vmem,) * 4,
        scratch_shapes=[pltpu.VMEM(x.shape, x.dtype) for x in operands]
        + [pltpu.VMEM((peers, features, halo), BF)] * 4
        + [
            pltpu.VMEM((LOW, ghosts), BF),
            pltpu.VMEM((LOW, faces), BF),
            pltpu.VMEM((LOW, faces), BF),
            pltpu.VMEM((16, faces), BF),
            pltpu.VMEM((16, faces), BF),
            pltpu.VMEM((16, ghosts), BF),
            pltpu.VMEM((2 * features, faces), BF),
            pltpu.VMEM((features, faces), F32),
            pltpu.VMEM((features, faces), BF),
            pltpu.VMEM((features, faces), F32),
            pltpu.VMEM((1, faces), F32),
            pltpu.VMEM((own_rows, LOW), F32),
            pltpu.VMEM((ghost_rows + own_rows, LOW), F32),
            pltpu.VMEM((own_rows, LOW), F32),
            pltpu.VMEM((features, 4 * features), F32),
            pltpu.VMEM((6, features, 128), F32),
            pltpu.VMEM((features, cells), F32),
            pltpu.VMEM((edge_number, PIECE, 128), BF),
            pltpu.VMEM((node_number, PIECE, 128), BF),
            pltpu.VMEM((count - 1, PIECE, 128), BF),
            pltpu.VMEM((count - 1, PIECE, 128), BF),
            pltpu.VMEM((PIECE, 128), BF),
            pltpu.VMEM((PIECE, 128), BF),
        ]
        + [dma((16,))]
        + [dma((3,))] * 4
        + [dma((4,))] * 2,
        compiler_params=pltpu.CompilerParams(
            collective_id=0, has_side_effects=True, vmem_limit_bytes=32 * 1024 * 1024
        ),
        name="layer",
    )(*(pltpu.with_memory_space_constraint(x, pltpu.HBM) for x in operands))
    vector = shape((1, features), F32)
    results = pl.pallas_call(
        functools.partial(unpack_kernel, 1.0 / math.sqrt(faces * count)),
        out_shape=(
            shape((features, cells), BF),
            shape((features, faces), BF),
            shape(edge_first.shape[::-1], F32),
            shape(edge_second.shape, F32),
            shape(node_first.shape[::-1], F32),
            shape(node_second.shape, F32),
        )
        + (vector,) * 6,
        in_specs=[vmem] * 4,
        out_specs=(vmem,) * 12,
        compiler_params=pltpu.CompilerParams(vmem_limit_bytes=16 * 1024 * 1024),
        name="unpack",
    )(state, edge_result, edge_total, node_total)
    state, edge_result, edge_first_sum, edge_second_sum, node_first_sum, node_second_sum, *vectors = results
    vectors = [v.reshape(-1) for v in vectors]
    return (
        state, edge_result, edge_first_sum.T, vectors[2], edge_second_sum, vectors[0], vectors[1],
        node_first_sum.T, vectors[5], node_second_sum, vectors[3], vectors[4],
    )


def solution(mesh):
    split = P(None, ("dom", "sub"))
    faces = P(("dom", "sub"))
    return jax.shard_map(
        functools.partial(on_device, mesh.shape["dom"], mesh.shape["sub"]),
        mesh=mesh,
        in_specs=(split, split, faces, faces, P(("dom", "sub"), None, None), split, split) + (P(),) * 9,
        out_specs=(split, split) + (P(),) * 10,
        check_vma=False,
    )
```

```python
import functools
import math

import jax
import jax.numpy as jnp
from jax import lax
from jax.experimental import pallas as pl
from jax.experimental.pallas import tpu as pltpu
from jax.sharding import PartitionSpec as P

EPSILON = 1e-05
MESH = pl.DeviceIdType.MESH
BF = jnp.bfloat16
F32 = jnp.float32
LOW = 256
PIECE = 16


def nn(a, b):
    return lax.dot_general(a, b, (((1,), (0,)), ((), ())), preferred_element_type=F32)


def nt(a, b):
    return lax.dot_general(a, b, (((1,), (1,)), ((), ())), preferred_element_type=F32)


def flip(a):
    return a.astype(F32).T


def standardize(values):
    centered = values - jnp.mean(values, axis=0, keepdims=True)
    spread = lax.rsqrt(jnp.mean(centered * centered, axis=0, keepdims=True) + EPSILON)
    return centered * spread, spread


def normalize_back(upstream, scaled, spread, gain):
    weighted = upstream * gain
    return spread * (
        weighted
        - jnp.mean(weighted, axis=0, keepdims=True)
        - scaled * jnp.mean(weighted * scaled, axis=0, keepdims=True)
    )


def lively_and_slope(linear):
    half = 0.5 * linear
    tilt = jnp.tanh(half)
    logistic = 0.5 + 0.5 * tilt
    lively = half + half * tilt
    return lively, logistic + lively * (1.0 - logistic)


def fold_lanes(values):
    total = values[:, :128]
    for begin in range(128, values.shape[1], 128):
        total = total + values[:, begin : begin + 128]
    return total


def stack_blocks(table):
    return jnp.concatenate([table[:, i : i + LOW] for i in range(0, table.shape[1], LOW)], axis=0)


def write_selector(selector, at, index):
    width = index.shape[1]
    low = jnp.bitwise_and(index, LOW - 1)
    offset = jnp.broadcast_to(low, (16, width)) - lax.broadcasted_iota(jnp.int32, (16, width), 0)
    offset = offset.astype(F32).astype(BF)
    one, zero = jnp.ones((16, width), BF), jnp.zeros((16, width), BF)
    for begin in range(0, LOW, 16):
        selector[begin : begin + 16, at] = jnp.where(offset == jnp.asarray(begin, BF), one, zero)


def choose(stacked, high, first, base):
    features = base.shape[0]
    high = jnp.broadcast_to(high, base.shape)
    for i in range(stacked.shape[0] // features):
        base = jnp.where(high == first + i, stacked[i * features : (i + 1) * features], base)
    return base


def spread_blocks(values, high, blocks):
    high = jnp.concatenate([high] * (values.shape[0] // 16), axis=0)
    zero = jnp.zeros(values.shape, values.dtype)
    return jnp.concatenate([jnp.where(high == jnp.asarray(i, BF), values, zero) for i in blocks], axis=0)


def high_part(index):
    return jnp.right_shift(index, 8)


def high_rows(index):
    return jnp.broadcast_to(high_part(index), (16, index.shape[1])).astype(F32).astype(BF)


def halo_peers(dom, sub):
    d, s = lax.axis_index("dom"), lax.axis_index("sub")
    for o in (0, 2, 1):
        for r in range(sub):
            if o == 1 and r == 0:
                continue
            t = lax.rem(s + r, sub)
            target = d + (o - 1)
            yield o, t, target, (target >= 0) & (target < dom)


def guarded(o, there, action):
    if o == 1:
        action()
    else:
        pl.when(there)(action)


def start_exchange(dom, sub, s, outgoing, incoming, send_sem, recv_sem, forward, only=(0, 2, 1)):
    for o, t, target, there in halo_peers(dom, sub):
        if o not in only:
            continue
        block = o if forward else 2 - o

        def start(block=block, t=t, target=target):
            pltpu.make_async_remote_copy(
                src_ref=outgoing.at[block * sub + t],
                dst_ref=incoming.at[block * sub + s],
                send_sem=send_sem.at[block],
                recv_sem=recv_sem.at[block],
                device_id=(target, t),
                device_id_type=MESH,
            ).start()

        guarded(o, there, start)


def reaches(dom):
    reach = 1
    while reach < dom - 1:
        yield reach
        reach *= 2


def announce(dom, sem, level, reach):
    d, s = lax.axis_index("dom"), lax.axis_index("sub")
    for row in (d - reach, d + reach):

        @pl.when((row >= 0) & (row < dom))
        def _():
            pl.semaphore_signal(sem.at[level], inc=1, device_id=(row, s), device_id_type=MESH)


def hear(dom, sem, level, reach):
    d = lax.axis_index("dom")
    number = jnp.where(d >= reach, 1, 0) + jnp.where(d + reach < dom, 1, 0)
    pl.semaphore_wait(sem.at[level], number)


def repeat(number, body):
    if number <= 32:
        for k in range(number):
            body(k)
    else:
        lax.fori_loop(0, number, lambda k, carry: (body(k), carry)[1], 0)


def clear_absent(dom, sub, s, incoming, forward):
    d = lax.axis_index("dom")
    incoming[sub + s] = jnp.zeros(incoming.shape[1:], incoming.dtype)
    for o in (0, 2):
        origin = d + 1 - o if forward else d + o - 1

        @pl.when((origin < 0) | (origin >= dom))
        def _():
            for u in range(sub):
                incoming[o * sub + u] = jnp.zeros(incoming.shape[1:], incoming.dtype)


def await_bytes(ref, sem):
    pltpu.make_async_copy(ref, ref, sem).wait()


def settle_exchange(dom, sub, blocks, sem, ahead, only=(1, 0, 2)):
    d = lax.axis_index("dom")
    for o in only:
        row = d + o - 1 if ahead else d + 1 - o
        number = sub - 1 if o == 1 else sub

        def finish(o=o, number=number):
            await_bytes(blocks.at[pl.ds(o * sub, number)], sem.at[o])

        guarded(o, (row >= 0) & (row < dom), finish)


def edge_owner(count, j):
    return count // 2 - 4 + j


def node_owner(count, j):
    return count // 2 + (j - 8 if j < 4 else j)


class Reduction:
    def __init__(self, count, sub, me, owner, is_owner, mine, packed, landing, reduced, result, sems):
        self.count, self.sub, self.me = count, sub, me
        self.number = packed.shape[0]
        self.owner, self.is_owner, self.mine = owner, is_owner, jnp.clip(mine, 0, self.number - 1)
        self.packed, self.landing, self.reduced, self.result, self.sems = packed, landing, reduced, result, sems

    def device(self, rank):
        return (rank // self.sub, lax.rem(rank, self.sub))

    def send_parts(self):
        for j in range(self.number):
            rank = self.owner(self.count, j)

            @pl.when(rank != self.me)
            def _():
                pltpu.make_async_remote_copy(
                    src_ref=self.packed.at[j],
                    dst_ref=self.landing.at[lax.rem(self.me - rank + self.count, self.count) - 1],
                    send_sem=self.sems.at[0],
                    recv_sem=self.sems.at[1],
                    device_id=self.device(rank),
                    device_id_type=MESH,
                ).start()

    def reduce(self):
        @pl.when(self.is_owner)
        def _():
            await_bytes(self.landing, self.sems.at[1])
            total = self.packed[self.mine].astype(F32) + jnp.sum(self.landing[...].astype(F32), axis=0)
            self.reduced[...] = total.astype(BF)
            self.result[self.mine] = total.astype(BF)

            def body(k):
                rank = lax.rem(self.me + 1 + lax.rem(k + self.count // 2, self.count - 1), self.count)
                pltpu.make_async_remote_copy(
                    src_ref=self.reduced,
                    dst_ref=self.result.at[self.mine],
                    send_sem=self.sems.at[2],
                    recv_sem=self.sems.at[3],
                    device_id=self.device(rank),
                    device_id_type=MESH,
                ).start()

            repeat(self.count - 1, body)

    def settle(self):
        @pl.when(self.is_owner)
        def _():
            await_bytes(self.packed.at[pl.ds(0, self.number - 1)], self.sems.at[0])
            await_bytes(self.landing, self.sems.at[2])
            await_bytes(self.result.at[pl.ds(0, self.number - 1)], self.sems.at[3])

        @pl.when(jnp.logical_not(self.is_owner))
        def _():
            await_bytes(self.packed, self.sems.at[0])
            await_bytes(self.result, self.sems.at[3])


def layer_kernel(
    dom, sub, chunk,
    node_in, edge_in, senders_in, receivers_in, index_in, node_cot_in, edge_cot_in,
    edge_first_in, edge_second_in, node_first_in, node_second_in,
    edge_bias_in, edge_gain_in, edge_shift_in, node_bias_in, node_gain_in,
    state_ref, edge_out_ref, edge_sum, node_sum,
    node_ref, edge_ref, senders_ref, receivers_ref, index_ref, node_cot_ref, edge_cot_ref,
    edge_first_ref, edge_second_ref, node_first_ref, node_second_ref,
    edge_bias_ref, edge_gain_ref, edge_shift_ref, node_bias_ref, node_gain_ref,
    outgoing, incoming, returning, returned,
    export_sel, sender_sel, receiver_sel, sender_high, receiver_high, export_high,
    stacked, slope, active, scaled_all, spread_all, summed, by_sender, by_receiver, grads, lanes, local,
    edge_packed, node_packed, edge_landing, node_landing, edge_reduced, node_reduced,
    load_sem, send_sem, recv_sem, back_send, back_recv,
    edge_sems, node_sems, known,
):
    features, cells = node_ref.shape
    faces = edge_ref.shape[1]
    peers, _, halo = outgoing.shape
    ghosts = peers * halo
    own_blocks = cells // LOW
    ghost_blocks = ghosts // LOW
    per = LOW // halo
    chunks = faces // chunk
    d, s = lax.axis_index("dom"), lax.axis_index("sub")
    count = dom * sub
    me = d * sub + s
    barrier = pltpu.get_barrier_semaphore()

    sources = [node_in, index_in, senders_in, receivers_in, edge_in, edge_first_in, edge_second_in,
               edge_bias_in, edge_gain_in, edge_shift_in, node_cot_in, node_first_in, node_second_in,
               node_bias_in, node_gain_in, edge_cot_in]
    targets = [node_ref, index_ref, senders_ref, receivers_ref, edge_ref, edge_first_ref, edge_second_ref,
               edge_bias_ref, edge_gain_ref, edge_shift_ref, node_cot_ref, node_first_ref, node_second_ref,
               node_bias_ref, node_gain_ref, edge_cot_ref]
    loads = [pltpu.make_async_copy(a, b, load_sem.at[i]) for i, (a, b) in enumerate(zip(sources, targets))]
    for load in loads:
        load.start()

    for o, t, target, there in halo_peers(dom, sub):

        def greet(t=t, target=target):
            pl.semaphore_signal(barrier, inc=1, device_id=(target, t), device_id_type=MESH)

        guarded(o, there, greet)
    neighbours = sub - 1 + jnp.where(d > 0, sub, 0) + jnp.where(d < dom - 1, sub, 0)
    clear_absent(dom, sub, s, incoming, True)
    clear_absent(dom, sub, s, returned, False)
    loads[0].wait()
    loads[1].wait()

    def halves(i):
        return pl.ds(pl.multiple_of(i * LOW, LOW), LOW)

    table = stack_blocks(node_ref[...])

    def pick(i):
        here = pl.ds(i * LOW, LOW)
        index = index_ref[:, here]
        write_selector(export_sel, here, index)
        export_high[:, here] = high_rows(index)
        picked = choose(nn(table, export_sel[:, here]), high_part(index), 0, jnp.zeros((features, LOW), F32))
        picked = picked.astype(BF)
        for p in range(per):
            outgoing[i * per + p] = picked[:, p * halo : (p + 1) * halo]

    third = ghost_blocks // 3
    for o in (0, 2, 1):
        for i in range(o * third, (o + 1) * third):
            pick(i)
        if o == 0:
            pl.semaphore_wait(barrier, neighbours)
        start_exchange(dom, sub, s, outgoing, incoming, send_sem, recv_sem, True, (o,))
    levels = list(enumerate(reaches(dom)))
    for level, reach in levels[:1]:
        announce(dom, known, level, reach)

    for load in loads[2:]:
        load.wait()
    edge_first_t = edge_first_ref[...]
    edge_first = flip(edge_first_t).astype(BF)
    edge_second = edge_second_ref[...]
    edge_second_t = flip(edge_second).astype(BF)
    vectors = [edge_bias_ref, edge_gain_ref, edge_shift_ref, node_bias_ref, node_gain_ref]
    columns = jnp.concatenate([v[...] for v in vectors] + [jnp.zeros((3, features), F32)], axis=0).T
    edge_bias, edge_gain, edge_shift, node_bias, node_gain = (columns[:, i : i + 1] for i in range(5))

    def span(c):
        return pl.ds(pl.multiple_of(c * chunk, chunk), chunk)

    everything = pl.ds(0, faces)

    def prepare(here):
        sender = senders_ref[:, here]
        receiver = receivers_ref[:, here]
        write_selector(sender_sel, here, sender)
        write_selector(receiver_sel, here, receiver)
        sender_high[:, here] = high_rows(sender)
        receiver_high[:, here] = high_rows(receiver)
        zero = jnp.zeros((features, faces), F32)
        received = choose(nn(table, receiver_sel[:, here]), high_part(receiver), 0, zero).astype(BF)
        sent = choose(nn(table, sender_sel[:, here]), high_part(sender), 0, zero).astype(BF)
        stacked[:features, here] = sent
        stacked[features:, here] = received
        slope[:, here] = nn(edge_first_t[:, features:], jnp.concatenate([received, edge_ref[:, here]], axis=0)) + edge_bias

    prepare(everything)
    for (level, reach), (after, further) in zip(levels[:1], levels[1:2]):
        hear(dom, known, level, reach)
        announce(dom, known, after, further)

    def ghosts_of(o):
        def block(i):
            return jnp.concatenate([incoming[i * per + p] for p in range(per)], axis=1)

        return jnp.concatenate([block(i) for i in range(o * third, (o + 1) * third)], axis=0)

    def gather_ghosts(o):
        settle_exchange(dom, sub, incoming, recv_sem, False, (o,))
        high = high_part(senders_ref[...])
        base = stacked[:features].astype(F32)
        return choose(nn(ghosts_of(o), sender_sel[...]), high, own_blocks + o * third, base).astype(BF)

    for o in (1, 0):
        stacked[:features] = gather_ghosts(o)
    settle_exchange(dom, sub, incoming, recv_sem, False, (2,))
    for (level, reach), (after, further) in zip(levels[1:], levels[2:]):
        hear(dom, known, level, reach)
        announce(dom, known, after, further)

    def forward(here):
        high = high_part(senders_ref[:, here])
        base = stacked[:features, here].astype(F32)
        sent = choose(nn(ghosts_of(2), sender_sel[:, here]), high, own_blocks + 2 * third, base).astype(BF)
        stacked[:features, here] = sent
        lively, steep = lively_and_slope(nn(edge_first_t[:, :features], sent) + slope[:, here])
        lively = lively.astype(BF)
        slope[:, here] = steep
        active[:, here] = lively
        scaled, spread = standardize(nn(edge_second_t, lively))
        scaled_all[:, here] = scaled
        spread_all[:, here] = spread
        message = (scaled * edge_gain + edge_shift).astype(BF)
        message = spread_blocks(message, receiver_high[:, here], range(own_blocks))
        summed[...] = nt(message, receiver_sel[:, here])

    forward(everything)

    def unstack(values):
        return jnp.concatenate([values[i : i + features] for i in range(0, values.shape[0], features)], axis=1)

    node_first_t = node_first_ref[...]
    node_first = flip(node_first_t).astype(BF)
    node_second_t = flip(node_second_ref[...]).astype(BF)
    node_input = jnp.concatenate([node_ref[...], unstack(summed[...]).astype(BF)], axis=0)
    node_lively, node_slope = lively_and_slope(nn(node_first_t, node_input) + node_bias)
    node_active = node_lively.astype(BF)
    node_scaled, node_spread = standardize(nn(node_second_t, node_active))
    upstream = node_cot_ref[...].astype(F32)
    node_delta = normalize_back(upstream, node_scaled, node_spread, node_gain).astype(BF)
    node_hidden = nn(node_second_ref[...], node_delta) * node_slope
    lanes[3] = fold_lanes(upstream * node_scaled)
    lanes[4] = fold_lanes(upstream)
    lanes[5] = fold_lanes(node_hidden)
    node_hidden = node_hidden.astype(BF)
    node_back = nn(node_first, node_hidden)
    local[...] = node_back[:features] + upstream
    toward = stack_blocks(node_back[features:].astype(BF))

    def columns_of(first):
        column = lax.broadcasted_iota(jnp.int32, (features, 128), 1)
        result = jnp.zeros((features, 128), F32)
        for i in range(3):
            result = jnp.where(column == i, jnp.sum(lanes[first + i], axis=1, keepdims=True), result)
        return result

    def pack(packed, begin, values):
        for j in range(values.shape[0] // PIECE):
            packed[begin + j] = values[j * PIECE : (j + 1) * PIECE].astype(BF)

    edge_number = edge_packed.shape[0]
    half = count // 2
    edge_mine = me - edge_owner(count, 0)
    edge_reduction = Reduction(
        count, sub, me, edge_owner, (edge_mine >= 0) & (edge_mine < edge_number), edge_mine,
        edge_packed, edge_landing, edge_reduced, edge_sum, edge_sems,
    )
    node_reduction = Reduction(
        count, sub, me, node_owner, ((me >= half - 8) & (me < half - 4)) | ((me >= half + 4) & (me < half + 8)),
        jnp.where(me < half, me - half + 8, me - half), node_packed, node_landing, node_reduced, node_sum, node_sems,
    )
    pack(node_packed, 0, nt(node_hidden, node_input))
    node_right = jnp.concatenate([nt(node_active, node_delta), columns_of(3)[:, :features]], axis=1)
    pack(node_packed, features // PIECE, node_right)
    for level, reach in levels[-1:]:
        hear(dom, known, level, reach)
    node_reduction.send_parts()


    def backward(here):
        zero = jnp.zeros((features, faces), F32)
        gathered = nn(toward, receiver_sel[:, here])
        delta = edge_cot_ref[:, here].astype(F32) + choose(gathered, high_part(receivers_ref[:, here]), 0, zero)
        scaled = scaled_all[:, here]
        lanes[0] = fold_lanes(delta * scaled)
        lanes[1] = fold_lanes(delta)
        edge_delta = normalize_back(delta, scaled, spread_all[:, here], edge_gain).astype(BF)
        grads[:, 192:] = nt(active[:, here], edge_delta)
        hidden = nn(edge_second, edge_delta) * slope[:, here]
        lanes[2] = fold_lanes(hidden)
        hidden = hidden.astype(BF)
        active[:, here] = hidden
        grads[:, :128] = nt(hidden, stacked[:, here])
        grads[:, 128:192] = nt(hidden, edge_ref[:, here])

    backward(everything)
    pack(edge_packed, 0, grads[:, :128])
    pack(edge_packed, features // PIECE, grads[:, 128:])
    edge_packed[edge_number - 1] = jnp.concatenate(
        [columns_of(0).T[:PIECE], jnp.zeros((PIECE, 128 - features), F32)], axis=1
    ).astype(BF)
    edge_reduction.send_parts()

    by_sender[...] = jnp.zeros(by_sender.shape, F32)
    by_receiver[...] = jnp.zeros(by_receiver.shape, F32)
    ghost_rows = ghost_blocks * features

    def scatter_ghosts(c, carry):
        here = span(c)
        values = spread_blocks(active[:, here], sender_high[:, here], range(own_blocks, own_blocks + ghost_blocks))
        by_sender[:ghost_rows] += nt(values, sender_sel[:, here])
        return carry

    lax.fori_loop(0, chunks, scatter_ghosts, 0)
    for i in range(ghost_blocks):
        back = nn(edge_first[:features], by_sender[i * features : (i + 1) * features].astype(BF)).astype(BF)
        for p in range(per):
            returning[i * per + p] = back[:, p * halo : (p + 1) * halo]
    start_exchange(dom, sub, s, returning, returned, back_send, back_recv, forward=False)

    def scatter_own(c, carry):
        here = span(c)
        hidden = active[:, here]
        by_sender[ghost_rows:] += nt(spread_blocks(hidden, sender_high[:, here], range(own_blocks)), sender_sel[:, here])
        by_receiver[...] += nt(spread_blocks(hidden, receiver_high[:, here], range(own_blocks)), receiver_sel[:, here])
        ahead = nn(edge_first[2 * features :], hidden)
        edge_out_ref[:, here] = (edge_cot_ref[:, here].astype(F32) + ahead).astype(BF)
        return carry

    lax.fori_loop(0, chunks, scatter_own, 0)
    both = jnp.concatenate([unstack(by_sender[ghost_rows:]), unstack(by_receiver[...])], axis=0).astype(BF)
    weights = jnp.concatenate([edge_first[:features], edge_first[features : 2 * features]], axis=1)
    local[...] += nn(weights, both)

    node_reduction.reduce()
    edge_reduction.reduce()
    settle_exchange(dom, sub, returned, back_recv, True)
    exported = jnp.concatenate([returned[k] for k in range(peers)], axis=1)
    exported = spread_blocks(exported, export_high[...], range(own_blocks))
    state_ref[...] = (local[...] + unstack(nt(exported, export_sel[...]))).astype(BF)
    settle_exchange(dom, sub, outgoing, send_sem, True)
    settle_exchange(dom, sub, returning, back_send, False)
    node_reduction.settle()
    edge_reduction.settle()


def unpack_kernel(
    factor, state_in, edge_in, edge_sum, node_sum,
    state_ref, edge_ref, edge_first_ref, edge_second_ref, node_first_ref, node_second_ref,
    edge_gain_ref, edge_shift_ref, edge_bias_ref, node_gain_ref, node_shift_ref, node_bias_ref,
):
    features = state_in.shape[0]
    pieces = features // PIECE
    state_ref[...] = state_in[...]
    edge_ref[...] = edge_in[...]

    def block(ref, begin):
        return jnp.concatenate([ref[begin + j] for j in range(pieces)], axis=0).astype(F32) * factor

    right = block(edge_sum, pieces)
    edge_first_ref[:, : 2 * features] = block(edge_sum, 0)
    edge_first_ref[:, 2 * features :] = right[:, :features]
    edge_second_ref[...] = right[:, features:]
    edge_vectors = edge_sum[2 * pieces].astype(F32) * factor
    node_first_ref[...] = block(node_sum, 0)
    right = block(node_sum, pieces)
    node_second_ref[...] = right[:, :features]
    node_vectors = right.T[features : features + 8]
    for i, ref in enumerate((edge_gain_ref, edge_shift_ref, edge_bias_ref)):
        ref[...] = edge_vectors[i : i + 1, :features]
    for i, ref in enumerate((node_gain_ref, node_shift_ref, node_bias_ref)):
        ref[...] = node_vectors[i : i + 1]


def on_device(
    dom, sub,
    node_state, edge_state, senders, receivers, send_index, node_cotangent, edge_cotangent,
    edge_first, edge_bias, edge_second, edge_gain, edge_shift, node_first, node_bias, node_second, node_gain,
):
    features, cells = node_state.shape
    faces = edge_state.shape[1]
    halo = send_index.shape[2]
    peers = 3 * sub
    ghosts = peers * halo
    count = dom * sub
    chunk = math.gcd(faces, 1536)
    edge_number = 2 * features // PIECE + 1
    node_number = 2 * features // PIECE
    vmem = pl.BlockSpec(memory_space=pltpu.VMEM)
    hbm = pl.BlockSpec(memory_space=pltpu.HBM)
    shape = jax.ShapeDtypeStruct
    dma = pltpu.SemaphoreType.DMA

    def line(vector):
        return vector.reshape(1, -1)

    operands = (
        node_state, edge_state, line(senders), line(receivers), line(send_index),
        node_cotangent, edge_cotangent, edge_first.T, edge_second, node_first.T, node_second,
        line(edge_bias), line(edge_gain), line(edge_shift), line(node_bias), line(node_gain),
    )
    own_rows = cells // LOW * features
    ghost_rows = ghosts // LOW * features
    state, edge_result, edge_total, node_total = pl.pallas_call(
        functools.partial(layer_kernel, dom, sub, chunk),
        out_shape=(
            shape((features, cells), BF),
            shape((features, faces), BF),
            shape((edge_number, PIECE, 128), BF),
            shape((node_number, PIECE, 128), BF),
        ),
        in_specs=[hbm] * 16,
        out_specs=(vmem,) * 4,
        scratch_shapes=[pltpu.VMEM(x.shape, x.dtype) for x in operands]
        + [pltpu.VMEM((peers, features, halo), BF)] * 4
        + [
            pltpu.VMEM((LOW, ghosts), BF),
            pltpu.VMEM((LOW, faces), BF),
            pltpu.VMEM((LOW, faces), BF),
            pltpu.VMEM((16, faces), BF),
            pltpu.VMEM((16, faces), BF),
            pltpu.VMEM((16, ghosts), BF),
            pltpu.VMEM((2 * features, faces), BF),
            pltpu.VMEM((features, faces), F32),
            pltpu.VMEM((features, faces), BF),
            pltpu.VMEM((features, faces), F32),
            pltpu.VMEM((1, faces), F32),
            pltpu.VMEM((own_rows, LOW), F32),
            pltpu.VMEM((ghost_rows + own_rows, LOW), F32),
            pltpu.VMEM((own_rows, LOW), F32),
            pltpu.VMEM((features, 4 * features), F32),
            pltpu.VMEM((6, features, 128), F32),
            pltpu.VMEM((features, cells), F32),
            pltpu.VMEM((edge_number, PIECE, 128), BF),
            pltpu.VMEM((node_number, PIECE, 128), BF),
            pltpu.VMEM((count - 1, PIECE, 128), BF),
            pltpu.VMEM((count - 1, PIECE, 128), BF),
            pltpu.VMEM((PIECE, 128), BF),
            pltpu.VMEM((PIECE, 128), BF),
        ]
        + [dma((16,))]
        + [dma((3,))] * 4
        + [dma((4,))] * 2
        + [pltpu.SemaphoreType.REGULAR((max(1, len(list(reaches(dom)))),))],
        compiler_params=pltpu.CompilerParams(
            collective_id=0, has_side_effects=True, vmem_limit_bytes=32 * 1024 * 1024
        ),
        name="layer",
    )(*(pltpu.with_memory_space_constraint(x, pltpu.HBM) for x in operands))
    vector = shape((1, features), F32)
    results = pl.pallas_call(
        functools.partial(unpack_kernel, 1.0 / math.sqrt(faces * count)),
        out_shape=(
            shape((features, cells), BF),
            shape((features, faces), BF),
            shape(edge_first.shape[::-1], F32),
            shape(edge_second.shape, F32),
            shape(node_first.shape[::-1], F32),
            shape(node_second.shape, F32),
        )
        + (vector,) * 6,
        in_specs=[vmem] * 4,
        out_specs=(vmem,) * 12,
        compiler_params=pltpu.CompilerParams(vmem_limit_bytes=16 * 1024 * 1024),
        name="unpack",
    )(state, edge_result, edge_total, node_total)
    state, edge_result, edge_first_sum, edge_second_sum, node_first_sum, node_second_sum, *vectors = results
    vectors = [v.reshape(-1) for v in vectors]
    return (
        state, edge_result, edge_first_sum.T, vectors[2], edge_second_sum, vectors[0], vectors[1],
        node_first_sum.T, vectors[5], node_second_sum, vectors[3], vectors[4],
    )


def solution(mesh):
    split = P(None, ("dom", "sub"))
    faces = P(("dom", "sub"))
    return jax.shard_map(
        functools.partial(on_device, mesh.shape["dom"], mesh.shape["sub"]),
        mesh=mesh,
        in_specs=(split, split, faces, faces, P(("dom", "sub"), None, None), split, split) + (P(),) * 9,
        out_specs=(split, split) + (P(),) * 10,
        check_vma=False,
    )
```

```python
import functools
import math

import jax
import jax.numpy as jnp
from jax import lax
from jax.experimental import pallas as pl
from jax.experimental.pallas import tpu as pltpu
from jax.sharding import PartitionSpec as P

EPSILON = 1e-05
MESH = pl.DeviceIdType.MESH
BF = jnp.bfloat16
F32 = jnp.float32
LOW = 256
PIECE = 8


def nn(a, b):
    return lax.dot_general(a, b, (((1,), (0,)), ((), ())), preferred_element_type=F32)


def nt(a, b):
    return lax.dot_general(a, b, (((1,), (1,)), ((), ())), preferred_element_type=F32)


def flip(a):
    return a.astype(F32).T


def standardize(values):
    centered = values - jnp.mean(values, axis=0, keepdims=True)
    spread = lax.rsqrt(jnp.mean(centered * centered, axis=0, keepdims=True) + EPSILON)
    return centered * spread, spread


def normalize_back(upstream, scaled, spread, gain):
    weighted = upstream * gain
    return spread * (
        weighted
        - jnp.mean(weighted, axis=0, keepdims=True)
        - scaled * jnp.mean(weighted * scaled, axis=0, keepdims=True)
    )


def lively_and_slope(half):
    tilt = jnp.tanh(half)
    tilted = half * tilt
    return half + tilted, (1.0 + tilt) + (half - tilted * tilt)


def pipeline(number, lag, stages):
    values = [None] * number
    for t in range(number + lag * (len(stages) - 1)):
        for k in reversed(range(len(stages))):
            c = t - k * lag
            if 0 <= c < number:
                values[c] = stages[k](c, values[c])


def fold_lanes(values):
    total = values[:, :128]
    for begin in range(128, values.shape[1], 128):
        total = total + values[:, begin : begin + 128]
    return total


def stack_blocks(table):
    return jnp.concatenate([table[:, i : i + LOW] for i in range(0, table.shape[1], LOW)], axis=0)


def write_selector(selector, at, index):
    width = index.shape[1]
    low = jnp.bitwise_and(index, LOW - 1)
    offset = jnp.broadcast_to(low, (16, width)) - lax.broadcasted_iota(jnp.int32, (16, width), 0)
    offset = offset.astype(F32).astype(BF)
    one, zero = jnp.ones((16, width), BF), jnp.zeros((16, width), BF)
    for begin in range(0, LOW, 16):
        selector[begin : begin + 16, at] = jnp.where(offset == jnp.asarray(begin, BF), one, zero)


def choose(stacked, features, high, first, base=None):
    blocks = [stacked[i : i + features] for i in range(0, stacked.shape[0], features)]
    if base is None:
        base, blocks, first = blocks[0], blocks[1:], first + 1
    high = jnp.broadcast_to(high, base.shape)
    for i, block in enumerate(blocks):
        base = jnp.where(high == first + i, block, base)
    return base


def spread_blocks(values, high, blocks):
    high = jnp.concatenate([high] * (values.shape[0] // 16), axis=0)
    zero = jnp.zeros(values.shape, values.dtype)
    return jnp.concatenate([jnp.where(high == jnp.asarray(i, BF), values, zero) for i in blocks], axis=0)


def split_products(chunks, groups):
    totals = [None] * len(groups)
    for values, high, turned in chunks:
        for g, blocks in enumerate(groups):
            part = nn(spread_blocks(values, high, blocks), turned)
            totals[g] = part if totals[g] is None else totals[g] + part
    return jnp.concatenate(totals, axis=0)


def halves_of(first, number):
    return range(first, first + number // 2), range(first + number // 2, first + number)


def high_part(index):
    return jnp.right_shift(index, 8)


def high_rows(index):
    return jnp.broadcast_to(high_part(index), (16, index.shape[1])).astype(F32).astype(BF)


def halo_peers(dom, sub):
    d, s = lax.axis_index("dom"), lax.axis_index("sub")
    for o in (0, 2, 1):
        for r in range(sub):
            if o == 1 and r == 0:
                continue
            t = lax.rem(s + r, sub)
            target = d + (o - 1)
            yield o, t, target, (target >= 0) & (target < dom)


def guarded(o, there, action):
    if o == 1:
        action()
    else:
        pl.when(there)(action)


def start_exchange(dom, sub, s, outgoing, incoming, send_sem, recv_sem, forward, only=(0, 2, 1)):
    for o, t, target, there in halo_peers(dom, sub):
        if o not in only:
            continue
        block = o if forward else 2 - o

        def start(block=block, t=t, target=target):
            pltpu.make_async_remote_copy(
                src_ref=outgoing.at[block * sub + t],
                dst_ref=incoming.at[block * sub + s],
                send_sem=send_sem.at[block],
                recv_sem=recv_sem.at[block],
                device_id=(target, t),
                device_id_type=MESH,
            ).start()

        guarded(o, there, start)


def reaches(dom):
    reach = 1
    while reach < dom - 1:
        yield reach
        reach *= 2


def announce(dom, sem, level, reach):
    d, s = lax.axis_index("dom"), lax.axis_index("sub")
    for row in (d - reach, d + reach):

        @pl.when((row >= 0) & (row < dom))
        def _():
            pl.semaphore_signal(sem.at[level], inc=1, device_id=(row, s), device_id_type=MESH)


def hear(dom, sem, level, reach):
    d = lax.axis_index("dom")
    number = jnp.where(d >= reach, 1, 0) + jnp.where(d + reach < dom, 1, 0)
    pl.semaphore_wait(sem.at[level], number)


def repeat(number, body):
    if number <= 32:
        for k in range(number):
            body(k)
    else:
        lax.fori_loop(0, number, lambda k, carry: (body(k), carry)[1], 0)


def clear_absent(dom, sub, s, incoming, forward):
    d = lax.axis_index("dom")
    incoming[sub + s] = jnp.zeros(incoming.shape[1:], incoming.dtype)
    for o in (0, 2):
        origin = d + 1 - o if forward else d + o - 1

        @pl.when((origin < 0) | (origin >= dom))
        def _():
            for u in range(sub):
                incoming[o * sub + u] = jnp.zeros(incoming.shape[1:], incoming.dtype)


def await_bytes(ref, sem):
    pltpu.make_async_copy(ref, ref, sem).wait()


def settle_exchange(dom, sub, blocks, sem, ahead, only=(1, 0, 2)):
    d = lax.axis_index("dom")
    for o in only:
        row = d + o - 1 if ahead else d + 1 - o
        number = sub - 1 if o == 1 else sub

        def finish(o=o, number=number):
            await_bytes(blocks.at[pl.ds(o * sub, number)], sem.at[o])

        guarded(o, (row >= 0) & (row < dom), finish)


def edge_owner(count, j):
    return 2 * j + 1


def node_owner(count, j):
    return count // 2 - 8 + j


def vector_owner(count, j):
    return count // 2 - 1


class Reduction:
    def __init__(self, count, sub, me, owner, is_owner, mine, packed, landing, reduced, result, sems):
        self.count, self.sub, self.me = count, sub, me
        self.number = packed.shape[0]
        self.owner, self.is_owner, self.mine = owner, is_owner, jnp.clip(mine, 0, self.number - 1)
        self.packed, self.landing, self.reduced, self.result, self.sems = packed, landing, reduced, result, sems

    def device(self, rank):
        return (rank // self.sub, lax.rem(rank, self.sub))

    def send_parts(self):
        for j in range(self.number):
            rank = self.owner(self.count, j)

            @pl.when(rank != self.me)
            def _():
                pltpu.make_async_remote_copy(
                    src_ref=self.packed.at[j],
                    dst_ref=self.landing.at[lax.rem(self.me - rank + self.count, self.count) - 1],
                    send_sem=self.sems.at[0],
                    recv_sem=self.sems.at[1],
                    device_id=self.device(rank),
                    device_id_type=MESH,
                ).start()

    def reduce(self):
        @pl.when(self.is_owner)
        def _():
            await_bytes(self.landing, self.sems.at[1])
            total = self.packed[self.mine].astype(F32) + jnp.sum(self.landing[...].astype(F32), axis=0)
            self.reduced[...] = total.astype(BF)
            self.result[self.mine] = total.astype(BF)

            def body(k):
                rank = k + jnp.where(k >= self.me, 1, 0)
                pltpu.make_async_remote_copy(
                    src_ref=self.reduced,
                    dst_ref=self.result.at[self.mine],
                    send_sem=self.sems.at[2],
                    recv_sem=self.sems.at[3],
                    device_id=self.device(rank),
                    device_id_type=MESH,
                ).start()

            repeat(self.count - 1, body)

    def settle(self):
        @pl.when(self.is_owner)
        def _():
            if self.number > 1:
                await_bytes(self.packed.at[pl.ds(0, self.number - 1)], self.sems.at[0])
                await_bytes(self.result.at[pl.ds(0, self.number - 1)], self.sems.at[3])
            await_bytes(self.landing, self.sems.at[2])

        @pl.when(jnp.logical_not(self.is_owner))
        def _():
            await_bytes(self.packed, self.sems.at[0])
            await_bytes(self.result, self.sems.at[3])


def layer_kernel(
    dom, sub,
    node_in, edge_in, senders_in, receivers_in, index_in, node_cot_in, edge_cot_in,
    edge_first_in, edge_second_in, node_first_in, node_second_in,
    edge_bias_in, edge_gain_in, edge_shift_in, node_bias_in, node_gain_in,
    state_ref, edge_out_ref, edge_sum, node_sum, vector_sum,
    node_ref, edge_ref, senders_ref, receivers_ref, index_ref, node_cot_ref, edge_cot_ref,
    edge_first_ref, edge_second_ref, node_first_ref, node_second_ref,
    edge_bias_ref, edge_gain_ref, edge_shift_ref, node_bias_ref, node_gain_ref,
    outgoing, incoming, returning, returned,
    export_sel, sender_sel, receiver_sel, sender_turned, receiver_turned, sender_high, receiver_high, export_high,
    stacked, slope, active, scaled_all, spread_all, lanes, local,
    edge_packed, node_packed, vector_packed, edge_landing, node_landing, vector_landing,
    edge_reduced, node_reduced, vector_reduced,
    load_sem, send_sem, recv_sem, back_send, back_recv,
    edge_sems, node_sems, vector_sems, known,
):
    features, cells = node_ref.shape
    faces = edge_ref.shape[1]
    peers, _, halo = outgoing.shape
    ghosts = peers * halo
    own_blocks = cells // LOW
    ghost_blocks = ghosts // LOW
    per = LOW // halo
    d, s = lax.axis_index("dom"), lax.axis_index("sub")
    count = dom * sub
    me = d * sub + s
    barrier = pltpu.get_barrier_semaphore()

    sources = [node_in, index_in, senders_in, receivers_in, edge_in, edge_first_in, edge_second_in,
               edge_bias_in, edge_gain_in, edge_shift_in, node_cot_in, node_first_in, node_second_in,
               node_bias_in, node_gain_in, edge_cot_in]
    targets = [node_ref, index_ref, senders_ref, receivers_ref, edge_ref, edge_first_ref, edge_second_ref,
               edge_bias_ref, edge_gain_ref, edge_shift_ref, node_cot_ref, node_first_ref, node_second_ref,
               node_bias_ref, node_gain_ref, edge_cot_ref]
    loads = [pltpu.make_async_copy(a, b, load_sem.at[i]) for i, (a, b) in enumerate(zip(sources, targets))]
    for load in loads:
        load.start()

    for o, t, target, there in halo_peers(dom, sub):

        def greet(t=t, target=target):
            pl.semaphore_signal(barrier, inc=1, device_id=(target, t), device_id_type=MESH)

        guarded(o, there, greet)
    neighbours = sub - 1 + jnp.where(d > 0, sub, 0) + jnp.where(d < dom - 1, sub, 0)
    clear_absent(dom, sub, s, incoming, True)
    clear_absent(dom, sub, s, returned, False)
    loads[0].wait()
    loads[1].wait()

    table = stack_blocks(node_ref[...])

    def pick(i):
        here = pl.ds(i * LOW, LOW)
        index = index_ref[:, here]
        write_selector(export_sel, here, index)
        export_high[:, here] = high_rows(index)
        picked = choose(nn(table, export_sel[:, here]), features, high_part(index), 0, jnp.zeros((features, LOW), F32))
        picked = picked.astype(BF)
        for p in range(per):
            outgoing[i * per + p] = picked[:, p * halo : (p + 1) * halo]

    third = ghost_blocks // 3
    for o in (0, 2, 1):
        for i in range(o * third, (o + 1) * third):
            pick(i)
        if o == 0:
            pl.semaphore_wait(barrier, neighbours)
        start_exchange(dom, sub, s, outgoing, incoming, send_sem, recv_sem, True, (o,))
    levels = list(enumerate(reaches(dom)))
    for level, reach in levels[:1]:
        announce(dom, known, level, reach)

    for load in loads[2:]:
        load.wait()
    edge_first_t = edge_first_ref[...]
    edge_first = flip(edge_first_t).astype(BF)
    edge_half_t = edge_first_t * jnp.asarray(0.5, BF)
    edge_second = edge_second_ref[...]
    edge_second_t = flip(edge_second).astype(BF)
    edge_second_half = edge_second * jnp.asarray(0.5, BF)
    vectors = [edge_bias_ref, edge_gain_ref, edge_shift_ref, node_bias_ref, node_gain_ref]
    columns = jnp.concatenate([v[...] for v in vectors] + [jnp.zeros((3, features), F32)], axis=0).T
    edge_bias, edge_gain, edge_shift, node_bias, node_gain = (columns[:, i : i + 1] for i in range(5))

    step = math.gcd(faces, 512)
    steps = faces // step

    def block(c):
        return pl.ds(c * step, step)

    def gather_own(c, _):
        here = block(c)
        sender = senders_ref[:, here]
        receiver = receivers_ref[:, here]
        write_selector(receiver_sel, here, receiver)
        receiver_high[:, here] = high_rows(receiver)
        received = choose(nn(table, receiver_sel[:, here]), features, high_part(receiver), 0).astype(BF)
        stacked[features:, here] = received
        write_selector(sender_sel, here, sender)
        sender_high[:, here] = high_rows(sender)
        stacked[:features, here] = choose(nn(table, sender_sel[:, here]), features, high_part(sender), 0).astype(BF)
        return received

    def first_half(c, received):
        here = block(c)
        stack = jnp.concatenate([received, edge_ref[:, here]], axis=0)
        slope[:, here] = nn(edge_half_t[:, features:], stack) + 0.5 * edge_bias

    pipeline(steps, 1, (gather_own, first_half))
    for (level, reach), (after, further) in zip(levels[:1], levels[1:2]):
        hear(dom, known, level, reach)
        announce(dom, known, after, further)

    def ghosts_of(o):
        def block(i):
            return jnp.concatenate([incoming[i * per + p] for p in range(per)], axis=1)

        return jnp.concatenate([block(i) for i in range(o * third, (o + 1) * third)], axis=0)

    def gather_ghosts(o, here):
        high = high_part(senders_ref[:, here])
        base = stacked[:features, here].astype(F32)
        sent = choose(nn(ghost_tables[o], sender_sel[:, here]), features, high, own_blocks + o * third, base).astype(BF)
        stacked[:features, here] = sent
        return sent

    for c in range(steps):
        receiver_turned[block(c)] = receiver_sel[:, block(c)].T
        sender_turned[block(c)] = sender_sel[:, block(c)].T
    ghost_tables = {}
    for o in (1, 2):
        settle_exchange(dom, sub, incoming, recv_sem, False, (o,))
        ghost_tables[o] = ghosts_of(o)
        for c in range(steps):
            gather_ghosts(o, block(c))
    settle_exchange(dom, sub, incoming, recv_sem, False, (0,))
    for (level, reach), (after, further) in zip(levels[1:], levels[2:]):
        hear(dom, known, level, reach)
        announce(dom, known, after, further)
    ghost_tables[0] = ghosts_of(0)

    forward_step = math.gcd(faces, 256)

    def forward_block(c):
        return pl.ds(c * forward_step, forward_step)

    def gather_last(c, _):
        return gather_ghosts(0, forward_block(c))

    def first_layer(c, sent):
        here = forward_block(c)
        lively, steep = lively_and_slope(nn(edge_half_t[:, :features], sent) + slope[:, here])
        lively = lively.astype(BF)
        slope[:, here] = steep
        active[:, here] = lively
        return lively

    def second_layer(c, lively):
        here = forward_block(c)
        scaled, spread = standardize(nn(edge_second_t, lively))
        scaled_all[:, here] = scaled
        spread_all[:, here] = spread
        message = (scaled * edge_gain + edge_shift).astype(BF)
        return message

    sums = [None, None]

    def add_messages(c, message):
        here = forward_block(c)
        for g, blocks in enumerate(halves_of(0, own_blocks)):
            part = nn(spread_blocks(message, receiver_high[:, here], blocks), receiver_turned[here])
            sums[g] = part if sums[g] is None else sums[g] + part

    pipeline(faces // forward_step, 3, (gather_last, first_layer, second_layer, add_messages))
    summed = jnp.concatenate(sums, axis=0)

    def unstack(values):
        return jnp.concatenate([values[i : i + features] for i in range(0, values.shape[0], features)], axis=1)

    node_first_t = node_first_ref[...]
    node_first = flip(node_first_t).astype(BF)
    node_second_t = flip(node_second_ref[...]).astype(BF)
    node_input = jnp.concatenate([node_ref[...], unstack(summed).astype(BF)], axis=0)
    node_lively, node_slope = lively_and_slope(0.5 * (nn(node_first_t, node_input) + node_bias))
    node_active = node_lively.astype(BF)
    node_scaled, node_spread = standardize(nn(node_second_t, node_active))
    upstream = node_cot_ref[...].astype(F32)
    node_delta = normalize_back(upstream, node_scaled, node_spread, node_gain).astype(BF)
    node_hidden = nn(node_second_ref[...], node_delta) * (0.5 * node_slope)
    lanes[3] = fold_lanes(upstream * node_scaled)
    lanes[4] = fold_lanes(upstream)
    lanes[5] = fold_lanes(node_hidden)
    node_hidden = node_hidden.astype(BF)
    node_back = nn(node_first, node_hidden)
    local[...] = node_back[:features] + upstream
    toward = stack_blocks(node_back[features:].astype(BF))

    def columns_of(first):
        column = lax.broadcasted_iota(jnp.int32, (features, 128), 1)
        result = jnp.zeros((features, 128), F32)
        for i in range(3):
            result = jnp.where(column == i, jnp.sum(lanes[first + i], axis=1, keepdims=True), result)
        return result

    def pack(packed, begin, values):
        for j in range(values.shape[0] // PIECE):
            packed[begin + j] = values[j * PIECE : (j + 1) * PIECE].astype(BF)

    edge_reduction = Reduction(
        count, sub, me, edge_owner, (me < 32) & (lax.rem(me, 2) == 1), me // 2,
        edge_packed, edge_landing, edge_reduced, edge_sum, edge_sems,
    )
    node_reduction = Reduction(
        count, sub, me, node_owner, (me >= count // 2 - 8) & (me < count // 2 + 8), me - (count // 2 - 8),
        node_packed, node_landing, node_reduced, node_sum, node_sems,
    )
    vector_reduction = Reduction(
        count, sub, me, vector_owner, me == vector_owner(count, 0), 0,
        vector_packed, vector_landing, vector_reduced, vector_sum, vector_sems,
    )
    pack(node_packed, 0, nt(node_hidden, node_input))
    node_right = jnp.concatenate([nt(node_active, node_delta), columns_of(3)[:, :features]], axis=1)
    pack(node_packed, features // PIECE, node_right)
    for level, reach in levels[-1:]:
        hear(dom, known, level, reach)
    node_reduction.send_parts()


    backward_step = math.gcd(faces, 3072)

    def backward_block(c):
        return pl.ds(c * backward_step, backward_step)

    def gather_toward(c, _):
        here = backward_block(c)
        return choose(nn(toward, receiver_sel[:, here]), features, high_part(receivers_ref[:, here]), 0)

    folded = []

    def norm_back(c, gathered):
        here = backward_block(c)
        delta = edge_cot_ref[:, here].astype(F32) + gathered
        scaled = scaled_all[:, here]
        folded.append([fold_lanes(delta * scaled), fold_lanes(delta)])
        return normalize_back(delta, scaled, spread_all[:, here], edge_gain).astype(BF)

    second_grads, first_grads, edge_grads = [], [], []

    def hidden_of(c, edge_delta):
        here = backward_block(c)
        hidden = nn(edge_second_half, edge_delta) * slope[:, here]
        second_grads.append(nt(active[:, here], edge_delta))
        folded[c].append(fold_lanes(hidden))
        hidden = hidden.astype(BF)
        active[:, here] = hidden
        return hidden

    def first_grad(c, hidden):
        here = backward_block(c)
        first_grads.append(nt(hidden, stacked[:, here]))
        edge_grads.append(nt(hidden, edge_ref[:, here]))

    pipeline(faces // backward_step, 1, (gather_toward, norm_back, hidden_of, first_grad))
    for i in range(3):
        lanes[i] = functools.reduce(jnp.add, [f[i] for f in folded])
    pack(edge_packed, 0, functools.reduce(jnp.add, first_grads))
    right = [functools.reduce(jnp.add, edge_grads), functools.reduce(jnp.add, second_grads)]
    pack(edge_packed, features // PIECE, jnp.concatenate(right, axis=1))
    edge_reduction.send_parts()
    vector_packed[0] = jnp.concatenate([columns_of(0).T[:PIECE], jnp.zeros((PIECE, 128 - features), F32)], axis=1).astype(BF)
    vector_reduction.send_parts()

    wide = math.gcd(faces, 1024)

    def pieces(turned, high):
        spans = [pl.ds(c * wide, wide) for c in range(faces // wide)]
        return [(active[:, here], high[:, here], turned[here]) for here in spans]

    by_ghost = split_products(pieces(sender_turned, sender_high), halves_of(own_blocks, ghost_blocks)).astype(BF)
    for i in range(ghost_blocks):
        back = nn(edge_first[:features], by_ghost[i * features : (i + 1) * features]).astype(BF)
        for p in range(per):
            returning[i * per + p] = back[:, p * halo : (p + 1) * halo]
    start_exchange(dom, sub, s, returning, returned, back_send, back_recv, forward=False)
    by_sender = split_products(pieces(sender_turned, sender_high), halves_of(0, own_blocks))
    by_receiver = split_products(pieces(receiver_turned, receiver_high), halves_of(0, own_blocks))
    node_reduction.reduce()
    for c in range(steps):
        here = block(c)
        ahead = nn(edge_first[2 * features :], active[:, here])
        edge_out_ref[:, here] = (edge_cot_ref[:, here].astype(F32) + ahead).astype(BF)
    both = jnp.concatenate([unstack(by_sender), unstack(by_receiver)], axis=0).astype(BF)
    weights = jnp.concatenate([edge_first[:features], edge_first[features : 2 * features]], axis=1)
    local[...] += nn(weights, both)

    edge_reduction.reduce()
    vector_reduction.reduce()
    settle_exchange(dom, sub, returned, back_recv, True)
    exported = jnp.concatenate([returned[k] for k in range(peers)], axis=1)
    arrived = [nt(spread_blocks(exported, export_high[...], g), export_sel[...]) for g in (range(own_blocks),)]
    state_ref[...] = (local[...] + unstack(jnp.concatenate(arrived, axis=0))).astype(BF)
    settle_exchange(dom, sub, outgoing, send_sem, True)
    settle_exchange(dom, sub, returning, back_send, False)
    node_reduction.settle()
    edge_reduction.settle()
    vector_reduction.settle()


def unpack_kernel(
    factor, state_in, edge_in, edge_sum, node_sum, vector_sum,
    state_ref, edge_ref, edge_first_ref, edge_second_ref, node_first_ref, node_second_ref,
    edge_gain_ref, edge_shift_ref, edge_bias_ref, node_gain_ref, node_shift_ref, node_bias_ref,
):
    features = state_in.shape[0]
    pieces = features // PIECE
    state_ref[...] = state_in[...]
    edge_ref[...] = edge_in[...]

    def block(ref, begin):
        return jnp.concatenate([ref[begin + j] for j in range(pieces)], axis=0).astype(F32) * factor

    right = block(edge_sum, pieces)
    edge_first_ref[:, : 2 * features] = block(edge_sum, 0)
    edge_first_ref[:, 2 * features :] = right[:, :features]
    edge_second_ref[...] = right[:, features:]
    edge_vectors = vector_sum[0].astype(F32) * factor
    node_first_ref[...] = block(node_sum, 0)
    right = block(node_sum, pieces)
    node_second_ref[...] = right[:, :features]
    node_vectors = right.T[features : features + 8]
    for i, ref in enumerate((edge_gain_ref, edge_shift_ref, edge_bias_ref)):
        ref[...] = edge_vectors[i : i + 1, :features]
    for i, ref in enumerate((node_gain_ref, node_shift_ref, node_bias_ref)):
        ref[...] = node_vectors[i : i + 1]


def on_device(
    dom, sub,
    node_state, edge_state, senders, receivers, send_index, node_cotangent, edge_cotangent,
    edge_first, edge_bias, edge_second, edge_gain, edge_shift, node_first, node_bias, node_second, node_gain,
):
    features, cells = node_state.shape
    faces = edge_state.shape[1]
    halo = send_index.shape[2]
    peers = 3 * sub
    ghosts = peers * halo
    count = dom * sub
    number = 2 * features // PIECE
    vmem = pl.BlockSpec(memory_space=pltpu.VMEM)
    hbm = pl.BlockSpec(memory_space=pltpu.HBM)
    shape = jax.ShapeDtypeStruct
    dma = pltpu.SemaphoreType.DMA

    def line(vector):
        return vector.reshape(1, -1)

    operands = (
        node_state, edge_state, line(senders), line(receivers), line(send_index),
        node_cotangent, edge_cotangent, edge_first.T, edge_second, node_first.T, node_second,
        line(edge_bias), line(edge_gain), line(edge_shift), line(node_bias), line(node_gain),
    )
    state, edge_result, *totals = pl.pallas_call(
        functools.partial(layer_kernel, dom, sub),
        out_shape=(
            shape((features, cells), BF),
            shape((features, faces), BF),
            shape((number, PIECE, 128), BF),
            shape((number, PIECE, 128), BF),
            shape((1, PIECE, 128), BF),
        ),
        in_specs=[hbm] * 16,
        out_specs=(vmem,) * 5,
        scratch_shapes=[pltpu.VMEM(x.shape, x.dtype) for x in operands]
        + [pltpu.VMEM((peers, features, halo), BF)] * 4
        + [
            pltpu.VMEM((LOW, ghosts), BF),
            pltpu.VMEM((LOW, faces), BF),
            pltpu.VMEM((LOW, faces), BF),
            pltpu.VMEM((faces, LOW), BF),
            pltpu.VMEM((faces, LOW), BF),
            pltpu.VMEM((16, faces), BF),
            pltpu.VMEM((16, faces), BF),
            pltpu.VMEM((16, ghosts), BF),
            pltpu.VMEM((2 * features, faces), BF),
            pltpu.VMEM((features, faces), F32),
            pltpu.VMEM((features, faces), BF),
            pltpu.VMEM((features, faces), F32),
            pltpu.VMEM((1, faces), F32),
            pltpu.VMEM((6, features, 128), F32),
            pltpu.VMEM((features, cells), F32),
            pltpu.VMEM((number, PIECE, 128), BF),
            pltpu.VMEM((number, PIECE, 128), BF),
            pltpu.VMEM((1, PIECE, 128), BF),
        ]
        + [pltpu.VMEM((count - 1, PIECE, 128), BF)] * 3
        + [pltpu.VMEM((PIECE, 128), BF)] * 3
        + [dma((16,))]
        + [dma((3,))] * 4
        + [dma((4,))] * 3
        + [pltpu.SemaphoreType.REGULAR((max(1, len(list(reaches(dom)))),))],
        compiler_params=pltpu.CompilerParams(
            collective_id=0, has_side_effects=True, vmem_limit_bytes=32 * 1024 * 1024
        ),
        name="layer",
    )(*(pltpu.with_memory_space_constraint(x, pltpu.HBM) for x in operands))
    vector = shape((1, features), F32)
    results = pl.pallas_call(
        functools.partial(unpack_kernel, 1.0 / math.sqrt(faces * count)),
        out_shape=(
            shape((features, cells), BF),
            shape((features, faces), BF),
            shape(edge_first.shape[::-1], F32),
            shape(edge_second.shape, F32),
            shape(node_first.shape[::-1], F32),
            shape(node_second.shape, F32),
        )
        + (vector,) * 6,
        in_specs=[vmem] * 5,
        out_specs=(vmem,) * 12,
        compiler_params=pltpu.CompilerParams(vmem_limit_bytes=16 * 1024 * 1024),
        name="unpack",
    )(state, edge_result, *totals)
    state, edge_result, edge_first_sum, edge_second_sum, node_first_sum, node_second_sum, *vectors = results
    vectors = [v.reshape(-1) for v in vectors]
    return (
        state, edge_result, edge_first_sum.T, vectors[2], edge_second_sum, vectors[0], vectors[1],
        node_first_sum.T, vectors[5], node_second_sum, vectors[3], vectors[4],
    )


def solution(mesh):
    split = P(None, ("dom", "sub"))
    faces = P(("dom", "sub"))
    return jax.shard_map(
        functools.partial(on_device, mesh.shape["dom"], mesh.shape["sub"]),
        mesh=mesh,
        in_specs=(split, split, faces, faces, P(("dom", "sub"), None, None), split, split) + (P(),) * 9,
        out_specs=(split, split) + (P(),) * 10,
        check_vma=False,
    )
```

```python
import functools
import math

import jax
import jax.numpy as jnp
from jax import lax
from jax.experimental import pallas as pl
from jax.experimental.pallas import tpu as pltpu
from jax.sharding import PartitionSpec as P

EPSILON = 1e-05
MESH = pl.DeviceIdType.MESH
BF = jnp.bfloat16
F32 = jnp.float32
LOW = 256
PIECE = 8


def nn(a, b):
    return lax.dot_general(a, b, (((1,), (0,)), ((), ())), preferred_element_type=F32)


def nt(a, b):
    return lax.dot_general(a, b, (((1,), (1,)), ((), ())), preferred_element_type=F32)


def flip(a):
    return a.astype(F32).T


def standardize(values):
    centered = values - jnp.mean(values, axis=0, keepdims=True)
    spread = lax.rsqrt(jnp.mean(centered * centered, axis=0, keepdims=True) + EPSILON)
    return centered * spread, spread


def normalize_back(upstream, scaled, spread, gain):
    weighted = upstream * gain
    return spread * (
        weighted
        - jnp.mean(weighted, axis=0, keepdims=True)
        - scaled * jnp.mean(weighted * scaled, axis=0, keepdims=True)
    )


def lively_and_slope(half):
    tilt = jnp.tanh(half)
    tilted = half * tilt
    return half + tilted, (1.0 + tilt) + (half - tilted * tilt)


def pipeline(number, lag, stages):
    values = [None] * number
    for t in range(number + lag * (len(stages) - 1)):
        for k in reversed(range(len(stages))):
            c = t - k * lag
            if 0 <= c < number:
                values[c] = stages[k](c, values[c])


def fold_lanes(values):
    total = values[:, :128]
    for begin in range(128, values.shape[1], 128):
        total = total + values[:, begin : begin + 128]
    return total


def stack_blocks(table):
    return jnp.concatenate([table[:, i : i + LOW] for i in range(0, table.shape[1], LOW)], axis=0)


def write_selector(selector, at, index):
    width = index.shape[1]
    low = jnp.bitwise_and(index, LOW - 1)
    offset = jnp.broadcast_to(low, (16, width)) - lax.broadcasted_iota(jnp.int32, (16, width), 0)
    offset = offset.astype(F32).astype(BF)
    one, zero = jnp.ones((16, width), BF), jnp.zeros((16, width), BF)
    for begin in range(0, LOW, 16):
        selector[begin : begin + 16, at] = jnp.where(offset == jnp.asarray(begin, BF), one, zero)


def choose(stacked, features, high, first, base=None):
    blocks = [stacked[i : i + features] for i in range(0, stacked.shape[0], features)]
    if base is None:
        base, blocks, first = blocks[0], blocks[1:], first + 1
    high = jnp.broadcast_to(high, base.shape)
    for i, block in enumerate(blocks):
        base = jnp.where(high == first + i, block, base)
    return base


def spread_blocks(values, high, blocks):
    high = jnp.concatenate([high] * (values.shape[0] // 16), axis=0)
    zero = jnp.zeros(values.shape, values.dtype)
    return jnp.concatenate([jnp.where(high == jnp.asarray(i, BF), values, zero) for i in blocks], axis=0)


def split_products(chunks, groups):
    totals = [None] * len(groups)
    for values, high, turned in chunks:
        for g, blocks in enumerate(groups):
            part = nn(spread_blocks(values, high, blocks), turned)
            totals[g] = part if totals[g] is None else totals[g] + part
    return jnp.concatenate(totals, axis=0)


def halves_of(first, number):
    return range(first, first + number // 2), range(first + number // 2, first + number)


def high_part(index):
    return jnp.right_shift(index, 8)


def high_rows(index):
    return jnp.broadcast_to(high_part(index), (16, index.shape[1])).astype(F32).astype(BF)


def halo_peers(dom, sub):
    d, s = lax.axis_index("dom"), lax.axis_index("sub")
    for o in (0, 2, 1):
        for r in range(sub):
            if o == 1 and r == 0:
                continue
            t = lax.rem(s + r, sub)
            target = d + (o - 1)
            yield o, t, target, (target >= 0) & (target < dom)


def guarded(o, there, action):
    if o == 1:
        action()
    else:
        pl.when(there)(action)


def start_exchange(dom, sub, s, outgoing, incoming, send_sem, recv_sem, forward, only=(0, 2, 1)):
    for o, t, target, there in halo_peers(dom, sub):
        if o not in only:
            continue
        block = o if forward else 2 - o

        def start(block=block, t=t, target=target):
            pltpu.make_async_remote_copy(
                src_ref=outgoing.at[block * sub + t],
                dst_ref=incoming.at[block * sub + s],
                send_sem=send_sem.at[block],
                recv_sem=recv_sem.at[block],
                device_id=(target, t),
                device_id_type=MESH,
            ).start()

        guarded(o, there, start)


def reaches(dom):
    reach = 1
    while reach < dom - 1:
        yield reach
        reach *= 2


def announce(dom, sem, level, reach):
    d, s = lax.axis_index("dom"), lax.axis_index("sub")
    for row in (d - reach, d + reach):

        @pl.when((row >= 0) & (row < dom))
        def _():
            pl.semaphore_signal(sem.at[level], inc=1, device_id=(row, s), device_id_type=MESH)


def hear(dom, sem, level, reach):
    d = lax.axis_index("dom")
    number = jnp.where(d >= reach, 1, 0) + jnp.where(d + reach < dom, 1, 0)
    pl.semaphore_wait(sem.at[level], number)


def repeat(number, body):
    if number <= 32:
        for k in range(number):
            body(k)
    else:
        lax.fori_loop(0, number, lambda k, carry: (body(k), carry)[1], 0)


def clear_absent(dom, sub, s, incoming, forward):
    d = lax.axis_index("dom")
    incoming[sub + s] = jnp.zeros(incoming.shape[1:], incoming.dtype)
    for o in (0, 2):
        origin = d + 1 - o if forward else d + o - 1

        @pl.when((origin < 0) | (origin >= dom))
        def _():
            for u in range(sub):
                incoming[o * sub + u] = jnp.zeros(incoming.shape[1:], incoming.dtype)


def await_bytes(ref, sem):
    pltpu.make_async_copy(ref, ref, sem).wait()


def settle_exchange(dom, sub, blocks, sem, ahead, only=(1, 0, 2)):
    d = lax.axis_index("dom")
    for o in only:
        row = d + o - 1 if ahead else d + 1 - o
        number = sub - 1 if o == 1 else sub

        def finish(o=o, number=number):
            await_bytes(blocks.at[pl.ds(o * sub, number)], sem.at[o])

        guarded(o, (row >= 0) & (row < dom), finish)


def vector_owner(count, j):
    return count // 2 - 1


class Reduction:
    def __init__(self, count, sub, me, owner, is_owner, mine, packed, landing, reduced, result, sems):
        self.count, self.sub, self.me = count, sub, me
        self.number = packed.shape[0]
        self.owner, self.is_owner, self.mine = owner, is_owner, jnp.clip(mine, 0, self.number - 1)
        self.packed, self.landing, self.reduced, self.result, self.sems = packed, landing, reduced, result, sems

    def device(self, rank):
        return (rank // self.sub, lax.rem(rank, self.sub))

    def send_parts(self):
        for j in range(self.number):
            rank = self.owner(self.count, j)

            @pl.when(rank != self.me)
            def _():
                pltpu.make_async_remote_copy(
                    src_ref=self.packed.at[j],
                    dst_ref=self.landing.at[lax.rem(self.me - rank + self.count, self.count) - 1],
                    send_sem=self.sems.at[0],
                    recv_sem=self.sems.at[1],
                    device_id=self.device(rank),
                    device_id_type=MESH,
                ).start()

    def reduce(self):
        @pl.when(self.is_owner)
        def _():
            await_bytes(self.landing, self.sems.at[1])
            total = self.packed[self.mine].astype(F32) + jnp.sum(self.landing[...].astype(F32), axis=0)
            self.reduced[...] = total.astype(BF)
            self.result[self.mine] = total.astype(BF)

            def body(k):
                rank = k + jnp.where(k >= self.me, 1, 0)
                pltpu.make_async_remote_copy(
                    src_ref=self.reduced,
                    dst_ref=self.result.at[self.mine],
                    send_sem=self.sems.at[2],
                    recv_sem=self.sems.at[3],
                    device_id=self.device(rank),
                    device_id_type=MESH,
                ).start()

            repeat(self.count - 1, body)

    def settle(self):
        @pl.when(self.is_owner)
        def _():
            if self.number > 1:
                await_bytes(self.packed.at[pl.ds(0, self.number - 1)], self.sems.at[0])
                await_bytes(self.result.at[pl.ds(0, self.number - 1)], self.sems.at[3])
            await_bytes(self.landing, self.sems.at[2])

        @pl.when(jnp.logical_not(self.is_owner))
        def _():
            await_bytes(self.packed, self.sems.at[0])
            await_bytes(self.result, self.sems.at[3])


def layer_kernel(
    dom, sub,
    node_in, edge_in, senders_in, receivers_in, index_in, node_cot_in, edge_cot_in,
    edge_first_in, edge_second_in, node_first_in, node_second_in,
    edge_bias_in, edge_gain_in, edge_shift_in, node_bias_in, node_gain_in,
    state_ref, edge_out_ref, edge_sum, node_sum, vector_sum,
    node_ref, edge_ref, senders_ref, receivers_ref, index_ref, node_cot_ref, edge_cot_ref,
    edge_first_ref, edge_second_ref, node_first_ref, node_second_ref,
    edge_bias_ref, edge_gain_ref, edge_shift_ref, node_bias_ref, node_gain_ref,
    outgoing, incoming, returning, returned,
    export_sel, sender_sel, receiver_sel, sender_turned, receiver_turned, sender_high, receiver_high, export_high,
    stacked, slope, active, scaled_all, spread_all, lanes, local,
    edge_packed, node_packed, vector_packed, edge_landing, node_landing, vector_landing,
    edge_reduced, node_reduced, vector_reduced,
    load_sem, send_sem, recv_sem, back_send, back_recv,
    edge_sems, node_sems, vector_sems, known,
):
    features, cells = node_ref.shape
    faces = edge_ref.shape[1]
    peers, _, halo = outgoing.shape
    ghosts = peers * halo
    own_blocks = cells // LOW
    ghost_blocks = ghosts // LOW
    per = LOW // halo
    d, s = lax.axis_index("dom"), lax.axis_index("sub")
    count = dom * sub
    me = d * sub + s
    barrier = pltpu.get_barrier_semaphore()

    sources = [node_in, index_in, senders_in, receivers_in, edge_in, edge_first_in, edge_second_in,
               edge_bias_in, edge_gain_in, edge_shift_in, node_cot_in, node_first_in, node_second_in,
               node_bias_in, node_gain_in, edge_cot_in]
    targets = [node_ref, index_ref, senders_ref, receivers_ref, edge_ref, edge_first_ref, edge_second_ref,
               edge_bias_ref, edge_gain_ref, edge_shift_ref, node_cot_ref, node_first_ref, node_second_ref,
               node_bias_ref, node_gain_ref, edge_cot_ref]
    loads = [pltpu.make_async_copy(a, b, load_sem.at[i]) for i, (a, b) in enumerate(zip(sources, targets))]
    for load in loads:
        load.start()

    for o, t, target, there in halo_peers(dom, sub):

        def greet(t=t, target=target):
            pl.semaphore_signal(barrier, inc=1, device_id=(target, t), device_id_type=MESH)

        guarded(o, there, greet)
    neighbours = sub - 1 + jnp.where(d > 0, sub, 0) + jnp.where(d < dom - 1, sub, 0)
    clear_absent(dom, sub, s, incoming, True)
    clear_absent(dom, sub, s, returned, False)
    loads[0].wait()
    loads[1].wait()

    table = stack_blocks(node_ref[...])

    def pick(i):
        here = pl.ds(i * LOW, LOW)
        index = index_ref[:, here]
        write_selector(export_sel, here, index)
        export_high[:, here] = high_rows(index)
        picked = choose(nn(table, export_sel[:, here]), features, high_part(index), 0, jnp.zeros((features, LOW), F32))
        picked = picked.astype(BF)
        for p in range(per):
            outgoing[i * per + p] = picked[:, p * halo : (p + 1) * halo]

    third = ghost_blocks // 3
    for o in (0, 2, 1):
        for i in range(o * third, (o + 1) * third):
            pick(i)
        if o == 0:
            pl.semaphore_wait(barrier, neighbours)
        start_exchange(dom, sub, s, outgoing, incoming, send_sem, recv_sem, True, (o,))
    levels = list(enumerate(reaches(dom)))
    for level, reach in levels[:1]:
        announce(dom, known, level, reach)

    for load in loads[2:]:
        load.wait()
    edge_first_t = edge_first_ref[...]
    edge_first = flip(edge_first_t).astype(BF)
    edge_half_t = edge_first_t * jnp.asarray(0.5, BF)
    edge_second = edge_second_ref[...]
    edge_second_t = flip(edge_second).astype(BF)
    edge_second_half = edge_second * jnp.asarray(0.5, BF)
    vectors = [edge_bias_ref, edge_gain_ref, edge_shift_ref, node_bias_ref, node_gain_ref]
    columns = jnp.concatenate([v[...] for v in vectors] + [jnp.zeros((3, features), F32)], axis=0).T
    edge_bias, edge_gain, edge_shift, node_bias, node_gain = (columns[:, i : i + 1] for i in range(5))

    step = math.gcd(faces, 512)
    steps = faces // step

    def block(c):
        return pl.ds(c * step, step)

    def gather_own(c, _):
        here = block(c)
        sender = senders_ref[:, here]
        receiver = receivers_ref[:, here]
        write_selector(receiver_sel, here, receiver)
        receiver_high[:, here] = high_rows(receiver)
        received = choose(nn(table, receiver_sel[:, here]), features, high_part(receiver), 0).astype(BF)
        stacked[features:, here] = received
        write_selector(sender_sel, here, sender)
        sender_high[:, here] = high_rows(sender)
        stacked[:features, here] = choose(nn(table, sender_sel[:, here]), features, high_part(sender), 0).astype(BF)
        return received

    def first_half(c, received):
        here = block(c)
        stack = jnp.concatenate([received, edge_ref[:, here]], axis=0)
        slope[:, here] = nn(edge_half_t[:, features:], stack) + 0.5 * edge_bias

    pipeline(steps, 1, (gather_own, first_half))
    for (level, reach), (after, further) in zip(levels[:1], levels[1:2]):
        hear(dom, known, level, reach)
        announce(dom, known, after, further)

    def ghosts_of(o):
        def block(i):
            return jnp.concatenate([incoming[i * per + p] for p in range(per)], axis=1)

        return jnp.concatenate([block(i) for i in range(o * third, (o + 1) * third)], axis=0)

    def gather_ghosts(o, here):
        high = high_part(senders_ref[:, here])
        base = stacked[:features, here].astype(F32)
        sent = choose(nn(ghost_tables[o], sender_sel[:, here]), features, high, own_blocks + o * third, base).astype(BF)
        stacked[:features, here] = sent
        return sent

    for c in range(steps):
        receiver_turned[block(c)] = receiver_sel[:, block(c)].T
        sender_turned[block(c)] = sender_sel[:, block(c)].T
    ghost_tables = {}
    for o in (1, 2):
        settle_exchange(dom, sub, incoming, recv_sem, False, (o,))
        ghost_tables[o] = ghosts_of(o)
        for c in range(steps):
            gather_ghosts(o, block(c))
    settle_exchange(dom, sub, incoming, recv_sem, False, (0,))
    for (level, reach), (after, further) in zip(levels[1:], levels[2:]):
        hear(dom, known, level, reach)
        announce(dom, known, after, further)
    ghost_tables[0] = ghosts_of(0)

    forward_step = math.gcd(faces, 256)

    def forward_block(c):
        return pl.ds(c * forward_step, forward_step)

    def gather_last(c, _):
        return gather_ghosts(0, forward_block(c))

    def first_layer(c, sent):
        here = forward_block(c)
        lively, steep = lively_and_slope(nn(edge_half_t[:, :features], sent) + slope[:, here])
        lively = lively.astype(BF)
        slope[:, here] = steep
        active[:, here] = lively
        return lively

    def second_layer(c, lively):
        here = forward_block(c)
        scaled, spread = standardize(nn(edge_second_t, lively))
        scaled_all[:, here] = scaled
        spread_all[:, here] = spread
        message = (scaled * edge_gain + edge_shift).astype(BF)
        return message

    sums = [None, None]

    def add_messages(c, message):
        here = forward_block(c)
        for g, blocks in enumerate(halves_of(0, own_blocks)):
            part = nn(spread_blocks(message, receiver_high[:, here], blocks), receiver_turned[here])
            sums[g] = part if sums[g] is None else sums[g] + part

    pipeline(faces // forward_step, 3, (gather_last, first_layer, second_layer, add_messages))
    summed = jnp.concatenate(sums, axis=0)

    def unstack(values):
        return jnp.concatenate([values[i : i + features] for i in range(0, values.shape[0], features)], axis=1)

    node_first_t = node_first_ref[...]
    node_first = flip(node_first_t).astype(BF)
    node_second_t = flip(node_second_ref[...]).astype(BF)
    node_input = jnp.concatenate([node_ref[...], unstack(summed).astype(BF)], axis=0)
    node_lively, node_slope = lively_and_slope(0.5 * (nn(node_first_t, node_input) + node_bias))
    node_active = node_lively.astype(BF)
    node_scaled, node_spread = standardize(nn(node_second_t, node_active))
    upstream = node_cot_ref[...].astype(F32)
    node_delta = normalize_back(upstream, node_scaled, node_spread, node_gain).astype(BF)
    node_hidden = nn(node_second_ref[...], node_delta) * (0.5 * node_slope)
    lanes[3] = fold_lanes(upstream * node_scaled)
    lanes[4] = fold_lanes(upstream)
    lanes[5] = fold_lanes(node_hidden)
    node_hidden = node_hidden.astype(BF)
    node_back = nn(node_first, node_hidden)
    local[...] = node_back[:features] + upstream
    toward = stack_blocks(node_back[features:].astype(BF))

    def columns_of(first):
        column = lax.broadcasted_iota(jnp.int32, (features, 128), 1)
        result = jnp.zeros((features, 128), F32)
        for i in range(3):
            result = jnp.where(column == i, jnp.sum(lanes[first + i], axis=1, keepdims=True), result)
        return result

    def pack(packed, begin, values):
        for j in range(values.shape[0] // PIECE):
            packed[begin + j] = values[j * PIECE : (j + 1) * PIECE].astype(BF)

    number = edge_packed.shape[0]

    def edge_owner(count, j):
        return 2 * (number - j) - 1

    def node_owner(count, j):
        return count // 2 - number // 2 + j

    node_mine = me - node_owner(count, 0)
    edge_reduction = Reduction(
        count, sub, me, edge_owner, (me < 2 * number) & (lax.rem(me, 2) == 1), number - 1 - me // 2,
        edge_packed, edge_landing, edge_reduced, edge_sum, edge_sems,
    )
    node_reduction = Reduction(
        count, sub, me, node_owner, (node_mine >= 0) & (node_mine < number), node_mine,
        node_packed, node_landing, node_reduced, node_sum, node_sems,
    )
    vector_reduction = Reduction(
        count, sub, me, vector_owner, me == vector_owner(count, 0), 0,
        vector_packed, vector_landing, vector_reduced, vector_sum, vector_sems,
    )
    pack(node_packed, 0, nt(node_hidden, node_input))
    node_right = jnp.concatenate([nt(node_active, node_delta), columns_of(3)[:, :features]], axis=1)
    pack(node_packed, features // PIECE, node_right)
    for level, reach in levels[-1:]:
        hear(dom, known, level, reach)
    node_reduction.send_parts()


    backward_step = math.gcd(faces, 3072)

    def backward_block(c):
        return pl.ds(c * backward_step, backward_step)

    def gather_toward(c, _):
        here = backward_block(c)
        return choose(nn(toward, receiver_sel[:, here]), features, high_part(receivers_ref[:, here]), 0)

    folded = []

    def norm_back(c, gathered):
        here = backward_block(c)
        delta = edge_cot_ref[:, here].astype(F32) + gathered
        scaled = scaled_all[:, here]
        folded.append([fold_lanes(delta * scaled), fold_lanes(delta)])
        return normalize_back(delta, scaled, spread_all[:, here], edge_gain).astype(BF)

    second_grads, first_grads, edge_grads = [], [], []

    def hidden_of(c, edge_delta):
        here = backward_block(c)
        hidden = nn(edge_second_half, edge_delta) * slope[:, here]
        second_grads.append(nt(active[:, here], edge_delta))
        folded[c].append(fold_lanes(hidden))
        hidden = hidden.astype(BF)
        active[:, here] = hidden
        return hidden

    def first_grad(c, hidden):
        here = backward_block(c)
        first_grads.append(nt(hidden, stacked[:, here]))
        edge_grads.append(nt(hidden, edge_ref[:, here]))

    pipeline(faces // backward_step, 1, (gather_toward, norm_back, hidden_of, first_grad))
    for i in range(3):
        lanes[i] = functools.reduce(jnp.add, [f[i] for f in folded])
    pack(edge_packed, 0, functools.reduce(jnp.add, first_grads))
    right = [functools.reduce(jnp.add, edge_grads), functools.reduce(jnp.add, second_grads)]
    pack(edge_packed, features // PIECE, jnp.concatenate(right, axis=1))
    edge_reduction.send_parts()
    vector_packed[0] = jnp.concatenate([columns_of(0).T[:PIECE], jnp.zeros((PIECE, 128 - features), F32)], axis=1).astype(BF)
    vector_reduction.send_parts()

    wide = math.gcd(faces, 1024)

    def pieces(turned, high):
        spans = [pl.ds(c * wide, wide) for c in range(faces // wide)]
        return [(active[:, here], high[:, here], turned[here]) for here in spans]

    by_ghost = split_products(pieces(sender_turned, sender_high), halves_of(own_blocks, ghost_blocks)).astype(BF)
    for i in range(ghost_blocks):
        back = nn(edge_first[:features], by_ghost[i * features : (i + 1) * features]).astype(BF)
        for p in range(per):
            returning[i * per + p] = back[:, p * halo : (p + 1) * halo]
    start_exchange(dom, sub, s, returning, returned, back_send, back_recv, forward=False)
    by_sender = split_products(pieces(sender_turned, sender_high), halves_of(0, own_blocks))
    by_receiver = split_products(pieces(receiver_turned, receiver_high), halves_of(0, own_blocks))
    node_reduction.reduce()
    for c in range(steps):
        here = block(c)
        ahead = nn(edge_first[2 * features :], active[:, here])
        edge_out_ref[:, here] = (edge_cot_ref[:, here].astype(F32) + ahead).astype(BF)
    both = jnp.concatenate([unstack(by_sender), unstack(by_receiver)], axis=0).astype(BF)
    weights = jnp.concatenate([edge_first[:features], edge_first[features : 2 * features]], axis=1)
    local[...] += nn(weights, both)

    edge_reduction.reduce()
    vector_reduction.reduce()
    settle_exchange(dom, sub, returned, back_recv, True)
    exported = jnp.concatenate([returned[k] for k in range(peers)], axis=1)
    arrived = [nt(spread_blocks(exported, export_high[...], g), export_sel[...]) for g in (range(own_blocks),)]
    state_ref[...] = (local[...] + unstack(jnp.concatenate(arrived, axis=0))).astype(BF)
    settle_exchange(dom, sub, outgoing, send_sem, True)
    settle_exchange(dom, sub, returning, back_send, False)
    node_reduction.settle()
    edge_reduction.settle()
    vector_reduction.settle()


def unpack_kernel(
    factor, state_in, edge_in, edge_sum, node_sum, vector_sum,
    state_ref, edge_ref, edge_first_ref, edge_second_ref, node_first_ref, node_second_ref,
    edge_gain_ref, edge_shift_ref, edge_bias_ref, node_gain_ref, node_shift_ref, node_bias_ref,
):
    features = state_in.shape[0]
    pieces = features // PIECE
    state_ref[...] = state_in[...]
    edge_ref[...] = edge_in[...]

    def block(ref, begin):
        return jnp.concatenate([ref[begin + j] for j in range(pieces)], axis=0).astype(F32) * factor

    right = block(edge_sum, pieces)
    edge_first_ref[:, : 2 * features] = block(edge_sum, 0)
    edge_first_ref[:, 2 * features :] = right[:, :features]
    edge_second_ref[...] = right[:, features:]
    edge_vectors = vector_sum[0].astype(F32) * factor
    node_first_ref[...] = block(node_sum, 0)
    right = block(node_sum, pieces)
    node_second_ref[...] = right[:, :features]
    node_vectors = right.T[features : features + 8]
    for i, ref in enumerate((edge_gain_ref, edge_shift_ref, edge_bias_ref)):
        ref[...] = edge_vectors[i : i + 1, :features]
    for i, ref in enumerate((node_gain_ref, node_shift_ref, node_bias_ref)):
        ref[...] = node_vectors[i : i + 1]


def on_device(
    dom, sub,
    node_state, edge_state, senders, receivers, send_index, node_cotangent, edge_cotangent,
    edge_first, edge_bias, edge_second, edge_gain, edge_shift, node_first, node_bias, node_second, node_gain,
):
    features, cells = node_state.shape
    faces = edge_state.shape[1]
    halo = send_index.shape[2]
    peers = 3 * sub
    ghosts = peers * halo
    count = dom * sub
    number = 2 * features // PIECE
    vmem = pl.BlockSpec(memory_space=pltpu.VMEM)
    hbm = pl.BlockSpec(memory_space=pltpu.HBM)
    shape = jax.ShapeDtypeStruct
    dma = pltpu.SemaphoreType.DMA

    def line(vector):
        return vector.reshape(1, -1)

    operands = (
        node_state, edge_state, line(senders), line(receivers), line(send_index),
        node_cotangent, edge_cotangent, edge_first.T, edge_second, node_first.T, node_second,
        line(edge_bias), line(edge_gain), line(edge_shift), line(node_bias), line(node_gain),
    )
    state, edge_result, *totals = pl.pallas_call(
        functools.partial(layer_kernel, dom, sub),
        out_shape=(
            shape((features, cells), BF),
            shape((features, faces), BF),
            shape((number, PIECE, 128), BF),
            shape((number, PIECE, 128), BF),
            shape((1, PIECE, 128), BF),
        ),
        in_specs=[hbm] * 16,
        out_specs=(vmem,) * 5,
        scratch_shapes=[pltpu.VMEM(x.shape, x.dtype) for x in operands]
        + [pltpu.VMEM((peers, features, halo), BF)] * 4
        + [
            pltpu.VMEM((LOW, ghosts), BF),
            pltpu.VMEM((LOW, faces), BF),
            pltpu.VMEM((LOW, faces), BF),
            pltpu.VMEM((faces, LOW), BF),
            pltpu.VMEM((faces, LOW), BF),
            pltpu.VMEM((16, faces), BF),
            pltpu.VMEM((16, faces), BF),
            pltpu.VMEM((16, ghosts), BF),
            pltpu.VMEM((2 * features, faces), BF),
            pltpu.VMEM((features, faces), F32),
            pltpu.VMEM((features, faces), BF),
            pltpu.VMEM((features, faces), F32),
            pltpu.VMEM((1, faces), F32),
            pltpu.VMEM((6, features, 128), F32),
            pltpu.VMEM((features, cells), F32),
            pltpu.VMEM((number, PIECE, 128), BF),
            pltpu.VMEM((number, PIECE, 128), BF),
            pltpu.VMEM((1, PIECE, 128), BF),
        ]
        + [pltpu.VMEM((count - 1, PIECE, 128), BF)] * 3
        + [pltpu.VMEM((PIECE, 128), BF)] * 3
        + [dma((16,))]
        + [dma((3,))] * 4
        + [dma((4,))] * 3
        + [pltpu.SemaphoreType.REGULAR((max(1, len(list(reaches(dom)))),))],
        compiler_params=pltpu.CompilerParams(
            collective_id=0, has_side_effects=True, vmem_limit_bytes=32 * 1024 * 1024
        ),
        name="layer",
    )(*(pltpu.with_memory_space_constraint(x, pltpu.HBM) for x in operands))
    vector = shape((1, features), F32)
    results = pl.pallas_call(
        functools.partial(unpack_kernel, 1.0 / math.sqrt(faces * count)),
        out_shape=(
            shape((features, cells), BF),
            shape((features, faces), BF),
            shape(edge_first.shape[::-1], F32),
            shape(edge_second.shape, F32),
            shape(node_first.shape[::-1], F32),
            shape(node_second.shape, F32),
        )
        + (vector,) * 6,
        in_specs=[vmem] * 5,
        out_specs=(vmem,) * 12,
        compiler_params=pltpu.CompilerParams(vmem_limit_bytes=16 * 1024 * 1024),
        name="unpack",
    )(state, edge_result, *totals)
    state, edge_result, edge_first_sum, edge_second_sum, node_first_sum, node_second_sum, *vectors = results
    vectors = [v.reshape(-1) for v in vectors]
    return (
        state, edge_result, edge_first_sum.T, vectors[2], edge_second_sum, vectors[0], vectors[1],
        node_first_sum.T, vectors[5], node_second_sum, vectors[3], vectors[4],
    )


def solution(mesh):
    split = P(None, ("dom", "sub"))
    faces = P(("dom", "sub"))
    return jax.shard_map(
        functools.partial(on_device, mesh.shape["dom"], mesh.shape["sub"]),
        mesh=mesh,
        in_specs=(split, split, faces, faces, P(("dom", "sub"), None, None), split, split) + (P(),) * 9,
        out_specs=(split, split) + (P(),) * 10,
        check_vma=False,
    )
```
